8 devices in a mesh: layer: 1 (over z), tp: 2 (over y), fsdp: 4 (over x, core).
Axes of the slice: x: 2, y: 2, z: 1, core: 2. Of those that a mesh axis runs over, the one named last changes fastest.
Arguments:
- wq_weight: float32 [2048, 2048], P(('layer', 'fsdp'), 'tp')
- wq_moment: float32 [2048, 2048], P(('layer', 'fsdp'), 'tp')
- wq_grad: bfloat16 [2048, 2048], P(('layer', 'fsdp'), 'tp')
- wq_factor: float32 [2048, 128], P(('layer', 'tp'))
- wk_weight: float32 [2048, 2048], P(('layer', 'fsdp'), 'tp')
- wk_moment: float32 [2048, 2048], P(('layer', 'fsdp'), 'tp')
- wk_grad: bfloat16 [2048, 2048], P(('layer', 'fsdp'), 'tp')
- wk_factor: float32 [2048, 128], P(('layer', 'tp'))
- wv_weight: float32 [2048, 2048], P(('layer', 'fsdp'), 'tp')
- wv_moment: float32 [2048, 2048], P(('layer', 'fsdp'), 'tp')
- wv_grad: bfloat16 [2048, 2048], P(('layer', 'fsdp'), 'tp')
- wv_factor: float32 [2048, 128], P(('layer', 'tp'))
- wo_weight: float32 [2048, 2048], P(('layer', 'fsdp'), 'tp')
- wo_moment: float32 [2048, 2048], P(('layer', 'fsdp'), 'tp')
- wo_grad: bfloat16 [2048, 2048], P(('layer', 'fsdp'), 'tp')
- wo_factor: float32 [2048, 128], P(('layer', 'tp'))
- gate_weight: float32 [8, 2048, 1408], P('layer', 'fsdp', 'tp')
- gate_moment: float32 [8, 2048, 1408], P('layer', 'fsdp', 'tp')
- gate_grad: bfloat16 [8, 2048, 1408], P('layer', 'fsdp', 'tp')
- gate_factor: float32 [8, 1408, 88], P('layer', 'tp')
- up_weight: float32 [8, 2048, 1408], P('layer', 'fsdp', 'tp')
- up_moment: float32 [8, 2048, 1408], P('layer', 'fsdp', 'tp')
- up_grad: bfloat16 [8, 2048, 1408], P('layer', 'fsdp', 'tp')
- up_factor: float32 [8, 1408, 88], P('layer', 'tp')
- down_weight: float32 [8, 1408, 2048], P('layer', 'fsdp', 'tp')
- down_moment: float32 [8, 1408, 2048], P('layer', 'fsdp', 'tp')
- down_grad: bfloat16 [8, 1408, 2048], P('layer', 'fsdp', 'tp')
- down_factor: float32 [8, 1408, 88], P('layer', 'fsdp')
Outputs:
- output 1: float32 [2048, 2048], P(('layer', 'fsdp'), 'tp')
- output 2: float32 [2048, 2048], P(('layer', 'fsdp'), 'tp')
- output 3: float32 [2048, 128], P(('layer', 'tp'))
- output 4: float32 [2048, 2048], P(('layer', 'fsdp'), 'tp')
- output 5: float32 [2048, 2048], P(('layer', 'fsdp'), 'tp')
- output 6: float32 [2048, 128], P(('layer', 'tp'))
- output 7: float32 [2048, 2048], P(('layer', 'fsdp'), 'tp')
- output 8: float32 [2048, 2048], P(('layer', 'fsdp'), 'tp')
- output 9: float32 [2048, 128], P(('layer', 'tp'))
- output 10: float32 [2048, 2048], P(('layer', 'fsdp'), 'tp')
- output 11: float32 [2048, 2048], P(('layer', 'fsdp'), 'tp')
- output 12: float32 [2048, 128], P(('layer', 'tp'))
- output 13: float32 [8, 2048, 1408], P('layer', 'fsdp', 'tp')
- output 14: float32 [8, 2048, 1408], P('layer', 'fsdp', 'tp')
- output 15: float32 [8, 1408, 88], P('layer', 'tp')
- output 16: float32 [8, 2048, 1408], P('layer', 'fsdp', 'tp')
- output 17: float32 [8, 2048, 1408], P('layer', 'fsdp', 'tp')
- output 18: float32 [8, 1408, 88], P('layer', 'tp')
- output 19: float32 [8, 1408, 2048], P('layer', 'fsdp', 'tp')
- output 20: float32 [8, 1408, 2048], P('layer', 'fsdp', 'tp')
- output 21: float32 [8, 1408, 88], P('layer', 'fsdp')
All inputs are finite; a program needn't handle non-finite values.
Results may differ from the reference program's by a relative error of at most 0.001.
Values are sent between devices in bfloat16 or wider.
A program may use at most 1 GiB of HBM per device.

```python
import math
import jax
import jax.numpy as jnp
from jax import lax

D = 2048
HEADS = 16
KV_HEADS = 16
HEAD = 128
FF = 1408
EXPERTS = 8
RANK_DIV = 16

MOMENTUM = 0.9
LEARN_RATE = 0.3
FULL_PREC = lax.Precision.HIGHEST


def draw_matrix(rand_key, n_rows, n_cols, n_side):
    sub_keys = jax.random.split(rand_key, 9)
    row_grad = jax.random.uniform(sub_keys[0], (n_rows, 1), jnp.float32, 0.5, 1.5)
    col_grad = jax.random.uniform(sub_keys[1], (1, n_cols), jnp.float32, 0.5, 1.5)
    row_mom = jax.random.uniform(sub_keys[2], (n_rows, 1), jnp.float32, 0.5, 1.5)
    col_mom = jax.random.uniform(sub_keys[3], (1, n_cols), jnp.float32, 0.5, 1.5)
    weight = jax.random.normal(sub_keys[4], (n_rows, n_cols), jnp.float32) * n_rows ** -0.5
    moment = 0.5 * jax.random.normal(sub_keys[5], (n_rows, n_cols), jnp.float32) * row_mom * col_mom
    gradient = (jax.random.normal(sub_keys[6], (n_rows, n_cols), jnp.float32) * row_grad * col_grad).astype(jnp.bfloat16)
    rank_cols = n_side // RANK_DIV
    col_fac = jax.random.uniform(sub_keys[7], (1, rank_cols), jnp.float32, 0.7, 1.3)
    factor = jax.random.normal(sub_keys[8], (n_side, rank_cols), jnp.float32) * col_fac * n_side ** -0.5
    return weight, moment, gradient, factor


def setup_inputs(seed: int = 0, part: int = 0) -> dict:
    part_key = jax.random.fold_in(jax.random.key(seed), part)
    mat_keys = jax.random.split(part_key, 7)
    q_width = HEADS * HEAD
    kv_width = KV_HEADS * HEAD
    drawn = [
        ('wq', draw_matrix(mat_keys[0], D, q_width, q_width)),
        ('wk', draw_matrix(mat_keys[1], D, kv_width, kv_width)),
        ('wv', draw_matrix(mat_keys[2], D, kv_width, kv_width)),
        ('wo', draw_matrix(mat_keys[3], q_width, D, D)),
        ('gate', jax.vmap(lambda sub_key: draw_matrix(sub_key, D, FF, FF))(jax.random.split(mat_keys[4], EXPERTS))),
        ('up', jax.vmap(lambda sub_key: draw_matrix(sub_key, D, FF, FF))(jax.random.split(mat_keys[5], EXPERTS))),
        ('down', jax.vmap(lambda sub_key: draw_matrix(sub_key, FF, D, FF))(jax.random.split(mat_keys[6], EXPERTS))),
    ]
    inputs = {}
    for prefix, arrays in drawn:
        for suffix, drawn_arr in zip(('weight', 'moment', 'grad', 'factor'), arrays):
            inputs[prefix + '_' + suffix] = drawn_arr
    return inputs


def dion_one(weight, moment, gradient, factor):
    mom_grad = moment + gradient.astype(jnp.float32)
    p_tilde = jnp.dot(mom_grad, factor, preferred_element_type=jnp.float32, precision=FULL_PREC)
    gram_mat = jnp.dot(p_tilde.T, p_tilde, preferred_element_type=jnp.float32, precision=FULL_PREC)
    chol_low = jnp.linalg.cholesky(gram_mat)
    p_orth = lax.linalg.triangular_solve(chol_low, p_tilde, left_side=False, lower=True, transpose_a=True)
    r_new = jnp.dot(mom_grad.T, p_orth, preferred_element_type=jnp.float32, precision=FULL_PREC)
    moment_new = mom_grad - (1.0 - MOMENTUM) * jnp.dot(p_orth, r_new.T, preferred_element_type=jnp.float32, precision=FULL_PREC)
    col_norm = jnp.sqrt(jnp.sum(r_new * r_new, axis=0, keepdims=True))
    factor_new = r_new / col_norm
    step_scale = LEARN_RATE * math.sqrt(mom_grad.shape[0] / mom_grad.shape[1])
    weight_new = weight - step_scale * jnp.dot(p_orth, factor_new.T, preferred_element_type=jnp.float32, precision=FULL_PREC)
    return weight_new, moment_new, factor_new


def dion_flip(weight, moment, gradient, factor):
    weight_new, moment_new, factor_new = dion_one(weight.T, moment.T, gradient.T, factor)
    return weight_new.T, moment_new.T, factor_new


def reference(wq_weight, wq_moment, wq_grad, wq_factor, wk_weight, wk_moment, wk_grad, wk_factor, wv_weight, wv_moment, wv_grad, wv_factor, wo_weight, wo_moment, wo_grad, wo_factor, gate_weight, gate_moment, gate_grad, gate_factor, up_weight, up_moment, up_grad, up_factor, down_weight, down_moment, down_grad, down_factor):
    wq_new = dion_one(wq_weight, wq_moment, wq_grad, wq_factor)
    wk_new = dion_one(wk_weight, wk_moment, wk_grad, wk_factor)
    wv_new = dion_one(wv_weight, wv_moment, wv_grad, wv_factor)
    wo_new = dion_one(wo_weight, wo_moment, wo_grad, wo_factor)
    gate_new = lax.map(lambda per_expert: dion_one(per_expert[0], per_expert[1], per_expert[2], per_expert[3]), (gate_weight, gate_moment, gate_grad, gate_factor))
    up_new = lax.map(lambda per_expert: dion_one(per_expert[0], per_expert[1], per_expert[2], per_expert[3]), (up_weight, up_moment, up_grad, up_factor))
    down_new = lax.map(lambda per_expert: dion_flip(per_expert[0], per_expert[1], per_expert[2], per_expert[3]), (down_weight, down_moment, down_grad, down_factor))
    return (wq_new[0], wq_new[1], wq_new[2], wk_new[0], wk_new[1], wk_new[2], wv_new[0], wv_new[1], wv_new[2], wo_new[0], wo_new[1], wo_new[2], gate_new[0], gate_new[1], gate_new[2], up_new[0], up_new[1], up_new[2], down_new[0], down_new[1], down_new[2])
```

```python
import math
import jax
import jax.numpy as jnp
from jax import lax
from jax.experimental import pallas as pl
from jax.experimental.pallas import tpu as pltpu
from jax.sharding import PartitionSpec as P

MOMENTUM = 0.9
LEARN_RATE = 0.3
FULL_PREC = lax.Precision.HIGHEST
LANES = 128
BF = jnp.bfloat16
F32 = jnp.float32


def split3(x):
    hi = x.astype(BF)
    rest = x - hi.astype(F32)
    mid = rest.astype(BF)
    low = (rest - mid.astype(F32)).astype(BF)
    return hi, mid, low


def eliminate(a_ref, li_ref, rank):
    lane = lax.broadcasted_iota(jnp.int32, (8, LANES), 1)
    for k0 in range(0, rank, 8):
        def step(kk, carry, k0=k0):
            k = k0 + kk
            row = a_ref[k]
            at_k = lane == k
            idx = jnp.full((8, LANES), k, jnp.int32)
            piv = jnp.take_along_axis(row, idx, axis=1)
            rinv = 1.0 / piv
            scaled = jnp.where(at_k, rinv, row * rinv)
            rs = 1.0 / jnp.sqrt(piv)
            li_ref[k] = jnp.where(at_k, rs, jnp.where(lane < k, row * rs, 0.0))
            for i in range(k0 + 1, rank):
                cur = a_ref[i]
                g = jnp.take_along_axis(cur, idx, axis=1)
                new = jnp.where(at_k, 0.0, cur) - g * scaled
                if i < k0 + 8:
                    new = jnp.where(i > k, new, cur)
                a_ref[i] = new
            return carry
        lax.fori_loop(0, 8, step, 0)


def chol_kernel(we_ref, wd_ref, le_ref, ld_ref, ae, ad):
    ae[...] = we_ref[...]
    ad[...] = wd_ref[...]
    for g in range(3):
        eliminate(ae.at[g], le_ref.at[g], 88)
    eliminate(ad, ld_ref, 128)


def chol_inverse(we, wd):
    return pl.pallas_call(
        chol_kernel,
        out_shape=(jax.ShapeDtypeStruct(we.shape, F32), jax.ShapeDtypeStruct(wd.shape, F32)),
        scratch_shapes=[pltpu.VMEM(we.shape, F32), pltpu.VMEM(wd.shape, F32)],
        name='chol_inverse',
    )(we, wd)


def pad_rows(x):
    rank, cols = x.shape
    if rank == LANES:
        return x
    return jnp.concatenate([x, jnp.zeros((LANES - rank, cols), F32)], axis=0)


def left_cat(ut):
    h, m, l = split3(pad_rows(ut).T)
    return jnp.concatenate([h, h, m, m, h, l], axis=1)


def right_cat(vt):
    h, m, l = split3(pad_rows(vt))
    return jnp.concatenate([l, h, m, h, m, h], axis=0)


def left_cat2(ut):
    h, m, l = split3(pad_rows(ut).T)
    return jnp.concatenate([h, l, m, m, h, h], axis=1)


def update_block(x_ref, m_ref, g_ref, ut, vt, dinv, x_out, m_out, scale):
    left = left_cat2(ut)
    b = m_ref[...] + g_ref[...].astype(F32)
    m_out[...] = b - (1.0 - MOMENTUM) * jnp.dot(left, right_cat(vt), preferred_element_type=F32)
    x_out[...] = x_ref[...] - scale * jnp.dot(left, right_cat(vt * dinv), preferred_element_type=F32)


def update_kernel(flips, scales, *refs):
    n = len(flips)
    ins, outs = refs[:6 * n], refs[6 * n:]
    for i in range(n):
        x_ref, m_ref, g_ref, pt_ref, rt_ref, d_ref = ins[6 * i:6 * i + 6]
        x_out, m_out, q_out = outs[3 * i:3 * i + 3]
        pt, rt, dinv = pt_ref[0], rt_ref[0], d_ref[0]
        ut, vt = (rt, pt) if flips[i] else (pt, rt)
        if len(x_ref.shape) == 3:
            x_ref, m_ref, g_ref, x_out, m_out, q_out = (r.at[0] for r in (x_ref, m_ref, g_ref, x_out, m_out, q_out))
        update_block(x_ref, m_ref, g_ref, ut, vt, dinv, x_out, m_out, scales[i])
        if len(x_ref.shape) == 2 and q_out.shape[0] == rt.shape[1]:
            q_out[...] = pad_rows(rt * dinv).T[:, :rt.shape[0]]


def expert_update(mats, scales):
    in_specs, out_specs, out_shape, args = [], [], [], []
    for x, m, g, pt, rt, d in mats:
        for arr in (x, m, g, pt, rt, d):
            in_specs.append(pl.BlockSpec((1,) + arr.shape[1:], lambda e: (e, 0, 0)))
            args.append(arr)
        q_shape = (rt.shape[0], rt.shape[2], rt.shape[1])
        for shape in (x.shape, x.shape, q_shape):
            out_specs.append(pl.BlockSpec((1,) + shape[1:], lambda e: (e, 0, 0)))
            out_shape.append(jax.ShapeDtypeStruct(shape, F32))

    def body(*refs):
        update_kernel((False, False, True), scales, *refs)

    return pl.pallas_call(
        body, grid=(8,), in_specs=in_specs, out_specs=out_specs, out_shape=out_shape,
        compiler_params=pltpu.CompilerParams(vmem_limit_bytes=60 * 2 ** 20),
        name='expert_update',
    )(*args)


def dense_body(scale, *refs):
    for i in range(4):
        x_ref, m_ref, g_ref, pt_ref, rt_ref, d_ref = refs[6 * i:6 * i + 6]
        x_out, m_out, q_out = refs[24 + 3 * i:27 + 3 * i]
        rt, dinv = rt_ref[0], d_ref[0]
        update_block(x_ref, m_ref, g_ref, pt_ref[0], rt, dinv, x_out, m_out, scale)
        part = pl.program_id(0)
        q_rows = q_out.shape[0]
        q_out[...] = (rt_ref[0, :, pl.ds(pl.multiple_of(part * q_rows, q_rows), q_rows)] * dinv).T


def dense_update(mats, scale):
    in_specs, out_specs, out_shape, args = [], [], [], []
    steps = 4
    for x, m, g, pt, rt, d in mats:
        rows, cols = x.shape
        blk = pl.BlockSpec((rows // steps, cols), lambda s: (s, 0))
        in_specs += [blk, blk, blk,
                     pl.BlockSpec((1, 128, rows // steps), lambda s: (0, 0, s)),
                     pl.BlockSpec(rt.shape, lambda s: (0, 0, 0)),
                     pl.BlockSpec(d.shape, lambda s: (0, 0, 0))]
        args += [x, m, g, pt, rt, d]
        out_specs += [blk, blk, pl.BlockSpec((cols // steps, 128), lambda s: (s, 0))]
        out_shape += [jax.ShapeDtypeStruct(x.shape, F32)] * 2 + [jax.ShapeDtypeStruct((cols, 128), F32)]

    def body(*refs):
        dense_body(scale, *refs)

    return pl.pallas_call(
        body, grid=(steps,), in_specs=in_specs, out_specs=out_specs, out_shape=out_shape,
        compiler_params=pltpu.CompilerParams(vmem_limit_bytes=60 * 2 ** 20),
        name='dense_update',
    )(*args)


def mat_mul(form, left_op, right_op):
    return jnp.einsum(form, left_op, right_op, preferred_element_type=F32, precision=FULL_PREC)


def solution(mesh):
    dense_w = P(('layer', 'fsdp'), 'tp')
    dense_f = P(('layer', 'tp'), None)
    stack_w = P('layer', 'fsdp', 'tp')
    stack_f = P('layer', 'tp', None)
    down_f = P('layer', 'fsdp', None)
    in_specs = (dense_w, dense_w, dense_w, dense_f) * 4 + (stack_w, stack_w, stack_w, stack_f) * 2 + (stack_w, stack_w, stack_w, down_f)
    out_specs = (dense_w, dense_w, dense_f) * 4 + (stack_w, stack_w, stack_f) * 2 + (stack_w, stack_w, down_f)

    def local_step(*blocks):
        mats = []
        for i in range(7):
            w, m, g, q = blocks[4 * i:4 * i + 4]
            if i < 4:
                w, m, g, q = w[None], m[None], g[None], q[None]
            b = m + g.astype(F32)
            flip = i == 6
            pt = mat_mul('bnr,bnm->brm' if flip else 'bnr,bmn->brm', q, b)
            pt = lax.psum(pt, 'fsdp' if flip else 'tp')
            gram = mat_mul('brm,bsm->brs', pt, pt)
            st = mat_mul('brm,bnm->brn' if flip else 'brm,bmn->brn', pt, b)
            gram, st = lax.psum((gram, st), 'tp' if flip else 'fsdp')
            mats.append([w, m, g, pt, st, gram])
        lane_pad = ((0, 0), (0, 0), (0, 0), (0, 40))
        we = jnp.stack([mats[i][5].transpose(1, 0, 2) for i in (4, 5, 6)])
        we = jnp.pad(we, lane_pad)
        wd = jnp.concatenate([mats[i][5] for i in (0, 1, 2, 3, 0, 1, 2, 3)]).transpose(1, 0, 2)
        le, ld = chol_inverse(we, wd)
        le = le.transpose(0, 2, 1, 3)[..., :88]
        ld = ld.transpose(1, 0, 2)
        ready = []
        sq = []
        for i in range(7):
            w, m, g, pt, st, _ = mats[i]
            linv = ld[i:i + 1] if i < 4 else le[i - 4]
            pt = mat_mul('brs,bsm->brm', linv, pt)
            rt = mat_mul('brs,bsn->brn', linv, st)
            ready.append([w, m, g, pt, rt])
            sq.append(jnp.sum(rt * rt, axis=2, keepdims=True))
        keep_sq = lax.psum(tuple(sq[:6]), 'tp')
        down_sq = lax.psum(sq[6], 'fsdp')
        for i in range(7):
            total = keep_sq[i] if i < 6 else down_sq
            ready[i].append(1.0 / jnp.sqrt(total))
        scale_e = LEARN_RATE * math.sqrt(2048 / 1408)
        results = []
        dense = [[r[0][0], r[1][0], r[2][0], r[3], r[4], r[5]] for r in ready[:4]]
        results.extend(dense_update(dense, LEARN_RATE))
        results.extend(expert_update(ready[4:], (scale_e,) * 3))
        return tuple(results)

    return jax.shard_map(local_step, mesh=mesh, in_specs=in_specs, out_specs=out_specs, check_vma=False)
```

```python
import math
import jax
import jax.numpy as jnp
from jax import lax
from jax.experimental import pallas as pl
from jax.experimental.pallas import tpu as pltpu
from jax.sharding import PartitionSpec as P

MOMENTUM = 0.9
LEARN_RATE = 0.3
LANES = 128
BF = jnp.bfloat16
F32 = jnp.float32
MIB = 2 ** 20
NN = (((1,), (0,)), ((), ()))
NT = (((1,), (1,)), ((), ()))
MESH = pl.DeviceIdType.MESH


def split3(x):
    hi = x.astype(BF)
    rest = x - hi.astype(F32)
    mid = rest.astype(BF)
    low = (rest - mid.astype(F32)).astype(BF)
    return hi, mid, low


def rows_to(x, rows):
    have, cols = x.shape
    if have == rows:
        return x
    return jnp.concatenate([x, jnp.zeros((rows - have, cols), x.dtype)], axis=0)


def dot6(left, right, dims):
    rank = left.shape[0]
    pad = -(-rank // 16) * 16
    lh, lm, ll = split3(rows_to(left, pad))
    rh, rm, rl = split3(right)
    with_h = lax.dot_general(jnp.concatenate([lh, lm, ll], axis=0), rh, dims, preferred_element_type=F32)
    with_m = lax.dot_general(jnp.concatenate([lh, lm], axis=0), rm, dims, preferred_element_type=F32)
    with_l = lax.dot_general(lh, rl, dims, preferred_element_type=F32)
    small = with_h[2 * pad:2 * pad + rank] + with_m[pad:pad + rank] + with_l[:rank]
    mid = with_h[pad:pad + rank] + with_m[:rank]
    return (small + mid) + with_h[:rank]


def exchange_kernel(*refs):
    em, eg, eq = refs[0:9:3], refs[1:9:3], refs[2:9:3]
    dm, dg, dq = refs[9:21:3], refs[10:21:3], refs[11:21:3]
    o_pk, o_pf, o_sf, o_sd, o_pd, o_sfd = refs[21:27]
    (mk, gk, qk, md, gd, qd, mw, gw, qw,
     pk, pk_in, pd, pd_c, pd_x, pf, sk, sk_c, sk_x, sf, sd, sd_in,
     pw, pw_in, sw, sw_c, sw_x, sfw,
     ld, ldw, ldq, out_sem, outw_sem, remote, remote_w) = refs[27:]
    t = lax.axis_index('tp')
    f = lax.axis_index('fsdp')
    c = lax.rem(f, 2)
    y_dev = {'tp': 1 - t}
    c_dev = {'fsdp': f + 1 - 2 * c}
    x_dev = {'fsdp': lax.rem(f + 2, 4)}
    bar = pltpu.get_barrier_semaphore()
    for dev in (y_dev, c_dev, x_dev):
        pl.semaphore_signal(bar, inc=1, device_id=dev, device_id_type=MESH)

    def expert_load(j, e, with_q):
        m_buf, g_buf, q_buf = (mk.at[j], gk.at[j], qk.at[j]) if j < 2 else (md, gd, qd)
        copies = [pltpu.make_async_copy(em[j].at[e], m_buf, ld.at[j, 0]),
                  pltpu.make_async_copy(eg[j].at[e], g_buf, ld.at[j, 1])]
        if with_q:
            copies.append(pltpu.make_async_copy(eq[j].at[e], q_buf, ld.at[j, 2]))
        return copies

    def start_all(copies):
        for cp in copies:
            cp.start()

    def wait_all(copies):
        for cp in copies:
            cp.wait()

    def dense_load(i, s):
        h, slot = lax.rem(s, 2), lax.rem(s, 2)
        rows = pl.ds(pl.multiple_of(h * 256, 256), 256)
        return [pltpu.make_async_copy(dm[i].at[rows], mw.at[slot], ldw.at[slot, 0]),
                pltpu.make_async_copy(dg[i].at[rows], gw.at[slot], ldw.at[slot, 1])]

    def dense_q(i, s):
        slot = lax.rem(s // 2, 2)
        return pltpu.make_async_copy(dq[i], qw.at[slot], ldq.at[slot])

    def dense_start(s, with_q):
        for i in range(4):
            @pl.when(s // 2 == i)
            def _():
                start_all(dense_load(i, s))
        if with_q:
            for i in range(4):
                @pl.when(jnp.logical_and(s // 2 == i, lax.rem(s, 2) == 0))
                def _():
                    dense_q(i, s).start()

    def send(src, dst, kind, e, dev):
        return pltpu.make_async_remote_copy(src_ref=src, dst_ref=dst, send_sem=remote.at[0, kind, e],
                                            recv_sem=remote.at[1, kind, e], device_id=dev, device_id_type=MESH)

    def send_w(src, dst, kind, i, dev):
        return pltpu.make_async_remote_copy(src_ref=src, dst_ref=dst, send_sem=remote_w.at[0, kind, i],
                                            recv_sem=remote_w.at[1, kind, i], device_id=dev, device_id_type=MESH)

    def r_pk(e, j):
        return send(pk.at[e, j], pk_in.at[e, j], j, e, y_dev)

    def r_pd_c(e):
        return send(pd.at[e, 1 - c], pd_c.at[e], 2, e, c_dev)

    def r_pd_x(e):
        return send(pd.at[e, c], pd_x.at[e], 3, e, x_dev)

    def r_pd_o(e):
        return send(pf.at[e, c], pf.at[e, c], 4, e, c_dev)

    def r_sk_c(e):
        return send(sk.at[e, 1 - c], sk_c.at[e], 5, e, c_dev)

    def r_sk_x(e):
        return send(sk.at[e, c], sk_x.at[e], 6, e, x_dev)

    def r_sk_o(e):
        return send(sf.at[e, c], sf.at[e, c], 7, e, c_dev)

    def r_sd(e):
        return send(sd.at[e], sd_in.at[e], 8, e, y_dev)

    def r_pw(i):
        return send_w(pw.at[i], pw_in.at[i], 0, i, y_dev)

    def r_sw_c(d):
        return send_w(sw.at[2 * d + 1 - c], sw_c.at[d], 1, d, c_dev)

    def r_sw_x(d):
        return send_w(sw.at[2 * d + c], sw_x.at[d], 2, d, x_dev)

    def r_sw_o(d):
        return send_w(sfw.at[2 * d + c], sfw.at[2 * d + c], 3, d, c_dev)

    def out_pk(e):
        return pltpu.make_async_copy(pk_in.at[e], o_pk.at[e], out_sem.at[0, e])

    def out_pf(e):
        return pltpu.make_async_copy(pf.at[e], o_pf.at[e], out_sem.at[1, e])

    def out_sf(e):
        return pltpu.make_async_copy(sf.at[e], o_sf.at[e], out_sem.at[2, e])

    def out_sd(e):
        return pltpu.make_async_copy(sd_in.at[e], o_sd.at[e], out_sem.at[3, e])

    def out_pw(i):
        return pltpu.make_async_copy(pw_in.at[i], o_pd.at[i], outw_sem.at[0, i])

    def out_sfw(i):
        return pltpu.make_async_copy(sfw.at[i], o_sfd.at[i], outw_sem.at[1, i])

    def block(j):
        if j < 2:
            return mk[j] + gk[j].astype(F32)
        return md[...] + gd[...].astype(F32)

    dense_start(0, True)
    for j in range(3):
        start_all(expert_load(j, 0, True))
    pl.semaphore_wait(bar, 3)

    def dense_one(s, carry):
        slot = lax.rem(s, 2)
        i = s // 2

        @pl.when(s < 7)
        def _():
            dense_start(s + 1, True)
        wait_all(dense_load(0, s))

        @pl.when(slot == 0)
        def _():
            dense_q(0, s).wait()
        b = mw[slot] + gw[slot].astype(F32)
        cols = pl.ds(pl.multiple_of(slot * 256, 256), 256)
        pw[i, :, cols] = dot6(qw[lax.rem(i, 2)].T, b, NT)

        @pl.when(slot == 1)
        def _():
            r_pw(i).start()
        return carry

    lax.fori_loop(0, 8, dense_one, 0)

    def pd_mid(e):
        r_pd_c(e).wait_recv()
        pd[e, c] = pd[e, c] + pd_c[e]
        r_pd_x(e).start()

    def expert_one(e, carry):
        for j in range(3):
            wait_all(expert_load(j, e, True))
            q = qk[j] if j < 2 else qd[...]
            part = dot6(q, block(j), NN)

            @pl.when(e < 7)
            def _(j=j):
                start_all(expert_load(j, e + 1, True))
            if j < 2:
                pk[e, j] = part
                r_pk(e, j).start()
            else:
                pd[e, 0] = part[:, :512]
                pd[e, 1] = part[:, 512:]
                r_pd_c(e).start()

        @pl.when(e > 0)
        def _():
            pd_mid(e - 1)
        return carry

    lax.fori_loop(0, 8, expert_one, 0)
    dense_start(0, False)
    for j in range(3):
        start_all(expert_load(j, 0, False))
    pd_mid(7)

    def dense_two(s, carry):
        slot = lax.rem(s, 2)
        i = s // 2

        @pl.when(s < 7)
        def _():
            dense_start(s + 1, False)

        @pl.when(slot == 0)
        def _():
            r_pw(i).wait_recv()
            total = pw[i] + pw_in[i]
            pw_in[i] = total
            out_pw(i).start()
            sw[i, :, 1024:] = dot6(total, total, NT)
            sw[i, :, :1024] = jnp.zeros((128, 1024), F32)
        wait_all(dense_load(0, s))
        b = mw[slot] + gw[slot].astype(F32)
        cols = pl.ds(pl.multiple_of(slot * 256, 256), 256)
        sw[i, :, :1024] = sw[i, :, :1024] + dot6(pw_in[i, :, cols], b, NN)

        @pl.when(lax.rem(s, 4) == 3)
        def _():
            r_sw_c(s // 4).start()
        return carry

    lax.fori_loop(0, 8, dense_two, 0)
    for d in range(2):
        r_sw_c(d).wait_recv()
        sw[2 * d + c] = sw[2 * d + c] + sw_c[d]
        r_sw_x(d).start()

    def sk_mid(e):
        r_sk_c(e).wait_recv()
        sk[e, c] = sk[e, c] + sk_c[e]
        r_sk_x(e).start()

    def expert_two(e, carry):
        r_pd_x(e).wait_recv()
        pf[e, c] = pd[e, c] + pd_x[e]
        r_pd_o(e).start()
        for j in range(2):
            r_pk(e, j).wait_recv()
            total = pk[e, j] + pk_in[e, j]
            pk_in[e, j] = total
            wait_all(expert_load(j, e, False))
            sk[e, j, :, 768:] = dot6(total, rows_to(total, 128), NT)
            sk[e, j, :, :768] = dot6(total, rows_to(block(j), 768), NT)

            @pl.when(e < 7)
            def _(j=j):
                start_all(expert_load(j, e + 1, False))
        out_pk(e).start()
        r_sk_c(e).start()
        r_pd_o(e).wait_recv()
        out_pf(e).start()
        wait_all(expert_load(2, e, False))
        total = jnp.concatenate([pf[e, 0], pf[e, 1]], axis=1)
        sd[e, :, 384:] = dot6(total, rows_to(total, 128), NT)
        sd[e, :, :384] = dot6(total, rows_to(block(2), 384), NT)

        @pl.when(e < 7)
        def _():
            start_all(expert_load(2, e + 1, False))
        r_sd(e).start()
        sk_mid(e)
        return carry

    lax.fori_loop(0, 8, expert_two, 0)

    for d in range(2):
        r_sw_x(d).wait_recv()
        sfw[2 * d + c] = sw[2 * d + c] + sw_x[d]
        r_sw_o(d).start()
    for d in range(2):
        r_sw_o(d).wait_recv()
        out_sfw(2 * d).start()
        out_sfw(2 * d + 1).start()

    def finish_keep(e, carry):
        r_sk_x(e).wait_recv()
        sf[e, c] = sk[e, c] + sk_x[e]
        r_sk_o(e).start()
        return carry

    lax.fori_loop(0, 8, finish_keep, 0)

    def finish(e, carry):
        r_sk_o(e).wait_recv()
        out_sf(e).start()
        r_sd(e).wait_recv()
        sd_in[e] = sd[e] + sd_in[e]
        out_sd(e).start()
        return carry

    lax.fori_loop(0, 8, finish, 0)

    def drain(e, carry):
        for r in (r_pk(e, 0), r_pk(e, 1), r_pd_c(e), r_pd_x(e), r_pd_o(e), r_sk_c(e), r_sk_x(e), r_sk_o(e), r_sd(e)):
            r.wait_send()
        for o in (out_pk(e), out_pf(e), out_sf(e), out_sd(e)):
            o.wait()
        return carry

    lax.fori_loop(0, 8, drain, 0)
    for i in range(4):
        r_pw(i).wait_send()
        out_pw(i).wait()
        out_sfw(i).wait()
    for d in range(2):
        r_sw_c(d).wait_send()
        r_sw_x(d).wait_send()
        r_sw_o(d).wait_send()


def exchange(experts, dense):
    any_spec = pl.BlockSpec(memory_space=pl.ANY)
    args = [a for grp in experts for a in grp] + [a for grp in dense for a in grp]
    shapes = [(8, 2, 88, 512), (8, 2, 88, 512), (8, 2, 88, 896), (8, 88, 512), (4, 128, 512), (4, 128, 1152)]
    dma = pltpu.SemaphoreType.DMA

    def v(*shape, dtype=F32):
        return pltpu.VMEM(shape, dtype)

    scratch = [v(2, 704, 512), v(2, 704, 512, dtype=BF), v(2, 88, 704),
               v(352, 1024), v(352, 1024, dtype=BF), v(88, 352),
               v(2, 256, 1024), v(2, 256, 1024, dtype=BF), v(2, 1024, 128),
               v(8, 2, 88, 512), v(8, 2, 88, 512),
               v(8, 2, 88, 512), v(8, 88, 512), v(8, 88, 512), v(8, 2, 88, 512),
               v(8, 2, 88, 896), v(8, 88, 896), v(8, 88, 896), v(8, 2, 88, 896),
               v(8, 88, 512), v(8, 88, 512),
               v(4, 128, 512), v(4, 128, 512), v(4, 128, 1152), v(2, 128, 1152), v(2, 128, 1152), v(4, 128, 1152),
               dma((3, 3)), dma((2, 2)), dma((2,)), dma((4, 8)), dma((2, 4)), dma((2, 9, 8)), dma((2, 4, 4))]
    return pl.pallas_call(
        exchange_kernel,
        in_specs=[any_spec] * len(args), out_specs=[any_spec] * len(shapes),
        out_shape=[jax.ShapeDtypeStruct(s, F32) for s in shapes],
        scratch_shapes=scratch,
        compiler_params=pltpu.CompilerParams(collective_id=0, has_side_effects=True, vmem_limit_bytes=67043328),
        name='exchange',
    )(*args)


def eliminate(a_ref, li_ref, rank):
    lane = lax.broadcasted_iota(jnp.int32, (8, LANES), 1)
    for k0 in range(0, rank, 8):
        def step(kk, carry, k0=k0):
            k = k0 + kk
            row = a_ref[k]
            at_k = lane == k
            idx = jnp.full((8, LANES), k, jnp.int32)
            piv = jnp.take_along_axis(row, idx, axis=1)
            rinv = 1.0 / piv
            scaled = jnp.where(at_k, rinv, row * rinv)
            rs = 1.0 / jnp.sqrt(piv)
            li_ref[k] = jnp.where(at_k, rs, jnp.where(lane < k, row * rs, 0.0))
            for i in range(k0 + 1, rank):
                cur = a_ref[i]
                g = jnp.take_along_axis(cur, idx, axis=1)
                new = jnp.where(at_k, 0.0, cur) - g * scaled
                if i < k0 + 8:
                    new = jnp.where(i > k, new, cur)
                a_ref[i] = new
            return carry
        lax.fori_loop(0, 8, step, 0)


def factor_kernel(sf_ref, sd_ref, sw_ref, le_ref, lw_ref, rk_ref, rd_ref, rw_ref, nrm,
                  ae, aw, li, lw):
    for e in range(8):
        for j in range(2):
            ae[j, :, e, :] = sf_ref[e, j, :, 768:]
        ae[2, :, e, :] = sd_ref[e, :, 384:]
        aw[:, e, :] = sw_ref[e % 4, :, 1024:]
    for g in range(3):
        eliminate(ae.at[g], li.at[g], 88)
    eliminate(aw, lw, 128)
    lane = lax.broadcasted_iota(jnp.int32, (128, LANES), 1)
    nrm[...] = jnp.zeros((128, LANES), F32)

    def add_norm(rt, where):
        sq = rows_to(jnp.sum(rt * rt, axis=1, keepdims=True), 128)
        nrm[...] = jnp.where(lane == where, sq, nrm[...])

    for e in range(8):
        for j in range(3):
            inv = li[j, :, e, :]
            le_ref[e, j] = inv
            st = sf_ref[e, j, :, :768] if j < 2 else sd_ref[e, :, :384]
            rt = dot6(inv, rows_to(st, 128), NN)
            if j < 2:
                rk_ref[e, j] = rt
            else:
                rd_ref[e] = rt
            add_norm(rt, 8 * j + e)
    for i in range(4):
        inv = lw[:, i, :]
        lw_ref[i] = inv
        rt = dot6(inv, sw_ref[i, :, :1024], NN)
        rw_ref[i] = rt
        add_norm(rt, 24 + i)

def norm_kernel(nrm, dinv_ref, nrm_y, nrm_f, sems):
    t = lax.axis_index('tp')
    f = lax.axis_index('fsdp')
    bar = pltpu.get_barrier_semaphore()
    y_dev = {'tp': 1 - t}
    pl.semaphore_signal(bar, inc=1, device_id=y_dev, device_id_type=MESH)
    for k in range(1, 4):
        pl.semaphore_signal(bar, inc=1, device_id={'fsdp': lax.rem(f + k, 4)}, device_id_type=MESH)
    pl.semaphore_wait(bar, 4)
    copies = [pltpu.make_async_remote_copy(src_ref=nrm, dst_ref=nrm_y, send_sem=sems.at[0, 0], recv_sem=sems.at[1, 0],
                                           device_id=y_dev, device_id_type=MESH)]
    for k in range(1, 4):
        copies.append(pltpu.make_async_remote_copy(src_ref=nrm, dst_ref=nrm_f.at[k], send_sem=sems.at[0, k], recv_sem=sems.at[1, k],
                                                   device_id={'fsdp': lax.rem(f + k, 4)}, device_id_type=MESH))
    for cp in copies:
        cp.start()
    for cp in copies:
        cp.wait()
    own = nrm[...]
    over_f = jnp.zeros((128, LANES), F32)
    for dev in range(4):
        k = lax.rem(f - dev + 4, 4)
        term = jnp.where(k == 0, own, jnp.where(k == 1, nrm_f[1], jnp.where(k == 2, nrm_f[2], nrm_f[3])))
        over_f = over_f + term
    lane = lax.broadcasted_iota(jnp.int32, (128, LANES), 1)
    is_down = jnp.logical_and(lane >= 16, lane < 24)
    total = jnp.where(is_down, over_f, own + nrm_y[...])
    dinv_ref[...] = 1.0 / jnp.sqrt(total)


def factor(sf, sd, sw):
    shapes = [(8, 3, 88, 128), (4, 128, 128), (8, 2, 88, 768), (8, 88, 384), (4, 128, 1024), (128, 128)]
    def v(*shape):
        return pltpu.VMEM(shape, F32)

    spec = pl.BlockSpec(memory_space=pltpu.VMEM)
    return pl.pallas_call(
        factor_kernel, in_specs=[spec] * 3, out_specs=[spec] * 6,
        out_shape=[jax.ShapeDtypeStruct(s, F32) for s in shapes],
        scratch_shapes=[v(3, 88, 8, 128), v(128, 8, 128), v(3, 88, 8, 128), v(128, 8, 128)],
        compiler_params=pltpu.CompilerParams(vmem_limit_bytes=60 * MIB),
        name='factor',
    )(sf, sd, sw)


def norms(nrm):
    spec = pl.BlockSpec(memory_space=pltpu.VMEM)
    return pl.pallas_call(
        norm_kernel, in_specs=[spec], out_specs=spec, out_shape=jax.ShapeDtypeStruct((128, 128), F32),
        scratch_shapes=[pltpu.VMEM((128, 128), F32), pltpu.VMEM((4, 128, 128), F32), pltpu.SemaphoreType.DMA((2, 4))],
        compiler_params=pltpu.CompilerParams(collective_id=1, has_side_effects=True),
        name='norms',
    )(nrm)


def left_cat(ut):
    h, m, l = split3(rows_to(ut, LANES).T)
    return jnp.concatenate([h, l, m, m, h, h], axis=1)


def right_cat(vt):
    h, m, l = split3(rows_to(vt, LANES))
    return jnp.concatenate([l, h, m, h, m, h], axis=0)


def take_col(dinv_ref, rank, where):
    lane = lax.broadcasted_iota(jnp.int32, (rank, LANES), 1)
    return jnp.sum(jnp.where(lane == where, dinv_ref[:rank, :], 0.0), axis=1, keepdims=True)


def apply_update(x_ref, m_ref, g_ref, ut, vt, dinv, x_out, m_out, scale):
    left = left_cat(ut)
    b = m_ref[...] + g_ref[...].astype(F32)
    m_out[...] = b - (1.0 - MOMENTUM) * jnp.dot(left, right_cat(vt), preferred_element_type=F32)
    x_out[...] = x_ref[...] - scale * jnp.dot(left, right_cat(vt * dinv), preferred_element_type=F32)


def expert_kernel(*refs):
    e = pl.program_id(0)
    pk, pf, le, rk, rd, dinv_ref = refs[9:15]
    scale = LEARN_RATE * math.sqrt(2048 / 1408)
    for j in range(3):
        x_ref, m_ref, g_ref = (r.at[0] for r in refs[3 * j:3 * j + 3])
        x_out, m_out, q_out = (r.at[0] for r in refs[15 + 3 * j:18 + 3 * j])
        dinv = take_col(dinv_ref, 88, 8 * j + e)
        if j < 2:
            pt, rt = pk[0, j], rk[0, j, :, :704]
        else:
            pt, rt = jnp.concatenate([pf[0, 0], pf[0, 1]], axis=1), rd[0, :, :352]
        pt = dot6(le[0, j], rows_to(pt, LANES), NN)
        apply_update(x_ref, m_ref, g_ref, rt, pt, dinv, x_out, m_out, scale)
        q_out[...] = rt * dinv


def expert_update(mats, sums):
    def blk(a):
        n = len(a.shape)
        return pl.BlockSpec((1,) + a.shape[1:], lambda e: (e,) + (0,) * (n - 1))

    args = [a for grp in mats for a in grp] + list(sums)
    in_specs = [blk(a) for a in args[:-1]] + [pl.BlockSpec((128, 128), lambda e: (0, 0))]
    out_shape = []
    for x, _, _ in mats:
        q_shape = (8, 88, x.shape[1])
        out_shape += [jax.ShapeDtypeStruct(s, F32) for s in (x.shape, x.shape, q_shape)]
    return pl.pallas_call(
        expert_kernel, grid=(8,), in_specs=in_specs, out_specs=[blk(o) for o in out_shape], out_shape=out_shape,
        compiler_params=pltpu.CompilerParams(vmem_limit_bytes=62 * MIB),
        name='expert_update',
    )(*args)


DENSE_STEPS = 4


def dense_kernel(*refs):
    pw, lw, rw, dinv_ref = refs[12:16]
    part = pl.program_id(0)
    for i in range(4):
        x_ref, m_ref, g_ref = refs[3 * i:3 * i + 3]
        x_out, m_out, q_out = refs[16 + 3 * i:19 + 3 * i]
        dinv = take_col(dinv_ref, 128, 24 + i)
        pt = dot6(lw[i], pw[i], NN)
        apply_update(x_ref, m_ref, g_ref, pt, rw[i], dinv, x_out, m_out, LEARN_RATE)
        q_rows = q_out.shape[0]
        q_out[...] = (rw[i, :, pl.ds(pl.multiple_of(part * q_rows, q_rows), q_rows)] * dinv).T


def dense_update(mats, pw, lw, rw, dinv):
    args = [a for grp in mats for a in grp] + [pw, lw, rw, dinv]
    rows, cols = mats[0][0].shape
    blk = pl.BlockSpec((rows // DENSE_STEPS, cols), lambda s: (s, 0))
    q_blk = pl.BlockSpec((cols // DENSE_STEPS, 128), lambda s: (s, 0))
    in_specs = [blk] * 12 + [pl.BlockSpec((4, 128, rows // DENSE_STEPS), lambda s: (0, 0, s)),
                             pl.BlockSpec(lw.shape, lambda s: (0, 0, 0)),
                             pl.BlockSpec(rw.shape, lambda s: (0, 0, 0)),
                             pl.BlockSpec(dinv.shape, lambda s: (0, 0))]
    w_out = jax.ShapeDtypeStruct((rows, cols), F32)
    return pl.pallas_call(
        dense_kernel, grid=(DENSE_STEPS,), in_specs=in_specs, out_specs=[blk, blk, q_blk] * 4,
        out_shape=[w_out, w_out, jax.ShapeDtypeStruct((cols, 128), F32)] * 4,
        compiler_params=pltpu.CompilerParams(vmem_limit_bytes=60 * MIB),
        name='dense_update',
    )(*args)


def solution(mesh):
    dense_w = P(('layer', 'fsdp'), 'tp')
    dense_f = P(('layer', 'tp'), None)
    stack_w = P('layer', 'fsdp', 'tp')
    stack_f = P('layer', 'tp', None)
    down_f = P('layer', 'fsdp', None)
    in_specs = (dense_w, dense_w, dense_w, dense_f) * 4 + (stack_w, stack_w, stack_w, stack_f) * 2 + (stack_w, stack_w, stack_w, down_f)
    out_specs = (dense_w, dense_w, dense_f) * 4 + (stack_w, stack_w, stack_f) * 2 + (stack_w, stack_w, down_f)

    def local_step(*blocks):
        dense = [blocks[4 * i:4 * i + 4] for i in range(4)]
        experts = []
        for i in (4, 5, 6):
            w, m, g, q = blocks[4 * i:4 * i + 4]
            if i < 6:
                w, m, g = (a.swapaxes(1, 2) for a in (w, m, g))
            experts.append((w, m, g, q.swapaxes(1, 2)))
        pk, pf, sf, sd, pw, sfw = exchange([grp[1:] for grp in experts], [grp[1:] for grp in dense])
        le, lw, rk, rd, rw, nrm = factor(sf, sd, sfw)
        dinv = norms(nrm)
        results = list(dense_update([grp[:3] for grp in dense], pw, lw, rw, dinv))
        out = list(expert_update([grp[:3] for grp in experts], (pk, pf, le, rk, rd, dinv)))
        for n in range(9):
            if n < 6 or n == 8:
                out[n] = out[n].swapaxes(1, 2)
        return tuple(results + out)

    return jax.shard_map(local_step, mesh=mesh, in_specs=in_specs, out_specs=out_specs, check_vma=False)
```

```python
import math
import jax
import jax.numpy as jnp
from jax import lax
from jax.experimental import pallas as pl
from jax.experimental.pallas import tpu as pltpu
from jax.sharding import PartitionSpec as P

MOMENTUM = 0.9
LEARN_RATE = 0.3
LANES = 128
BF = jnp.bfloat16
F32 = jnp.float32
MIB = 2 ** 20
NN = (((1,), (0,)), ((), ()))
NT = (((1,), (1,)), ((), ()))
MESH = pl.DeviceIdType.MESH


def split3(x):
    hi = x.astype(BF)
    rest = x - hi.astype(F32)
    mid = rest.astype(BF)
    low = (rest - mid.astype(F32)).astype(BF)
    return hi, mid, low


def rows_to(x, rows):
    have, cols = x.shape
    if have == rows:
        return x
    return jnp.concatenate([x, jnp.zeros((rows - have, cols), x.dtype)], axis=0)


def dot6(left, right, dims):
    rank = left.shape[0]
    pad = -(-rank // 16) * 16
    lh, lm, ll = split3(rows_to(left, pad))
    rh, rm, rl = split3(right)
    with_h = lax.dot_general(jnp.concatenate([lh, lm, ll], axis=0), rh, dims, preferred_element_type=F32)
    with_m = lax.dot_general(jnp.concatenate([lh, lm], axis=0), rm, dims, preferred_element_type=F32)
    with_l = lax.dot_general(lh, rl, dims, preferred_element_type=F32)
    small = with_h[2 * pad:2 * pad + rank] + with_m[pad:pad + rank] + with_l[:rank]
    mid = with_h[pad:pad + rank] + with_m[:rank]
    return (small + mid) + with_h[:rank]


def eliminate(a, li, rank):
    lane = lax.broadcasted_iota(jnp.int32, (8, LANES), 1)

    def pick(x, hit):
        return jnp.sum(jnp.where(hit, x, 0.0), axis=-1, keepdims=True)

    for k0 in range(0, rank, 8):
        def step(kk, carry, k0=k0):
            k = k0 + 2 * kk
            h0, h1 = lane == k, lane == k + 1
            r0, r1 = a[k], a[k + 1]
            v00, v01, v10, v11 = pick(r0, h0), pick(r0, h1), pick(r1, h0), pick(r1, h1)
            rinv0 = 1.0 / v00
            rs0 = 1.0 / jnp.sqrt(v00)
            s01 = v01 * rinv0
            sc0 = jnp.where(h0, rinv0, r0 * rinv0)
            li[k] = jnp.where(h0, rs0, jnp.where(lane < k, r0 * rs0, 0.0))
            piv1 = v11 - v10 * s01
            rinv1 = 1.0 / piv1
            rs1 = 1.0 / jnp.sqrt(piv1)
            r1 = jnp.where(h0, 0.0, r1) - v10 * sc0
            sc1 = jnp.where(h1, rinv1, r1 * rinv1)
            li[k + 1] = jnp.where(h1, rs1, jnp.where(lane < k + 1, r1 * rs1, 0.0))
            sc0 = jnp.where(h1, 0.0, sc0)

            def below(lo, n, masked):
                lane_n = lax.broadcasted_iota(jnp.int32, (n, 8, LANES), 2)
                g_hit0, g_hit1 = lane_n == k, lane_n == k + 1
                cur = a[lo:lo + n]
                g0 = pick(cur, g_hit0)
                g1 = pick(cur, g_hit1) - g0 * s01[None]
                new = jnp.where(jnp.logical_or(g_hit0, g_hit1), 0.0, cur) - g0 * sc0[None] - g1 * sc1[None]
                if masked:
                    row = lo + lax.broadcasted_iota(jnp.int32, (n, 8, LANES), 0)
                    new = jnp.where(row > k + 1, new, cur)
                a[lo:lo + n] = new

            below(k0, 8, True)
            if rank > k0 + 8:
                below(k0 + 8, rank - k0 - 8, False)
            return carry
        lax.fori_loop(0, 4, step, 0)


def exchange_kernel(*refs):
    em, eg, eq = refs[0:9:3], refs[1:9:3], refs[2:9:3]
    dm, dg, dq = refs[9:21:3], refs[10:21:3], refs[11:21:3]
    o_pk, o_pf, o_sf, o_sd, o_pd, o_sfd, o_nrm = refs[21:28]
    (mk, gk, qk, md, gd, qd, mw, gw, qw,
     pk, pk_in, pd, pd_c, pd_x, pf, sk, sk_c, sk_x, sf, sd, sd_in, wd, wd_in,
     pw, pw_in, sw, sw_c, sw_x, sfw, ae, li, aw, lw, nrm, nrm_y, nrm_d, nrm_f,
     ld, ldw, ldq, out_sem, outw_sem, remote, remote_w, remote_n) = refs[28:]
    t = lax.axis_index('tp')
    f = lax.axis_index('fsdp')
    c = lax.rem(f, 2)
    y_dev = {'tp': 1 - t}
    c_dev = {'fsdp': f + 1 - 2 * c}
    x_dev = {'fsdp': lax.rem(f + 2, 4)}
    xc_dev = {'fsdp': lax.rem(f + 3 - 2 * c, 4)}
    yc_dev = {'tp': 1 - t, 'fsdp': f + 1 - 2 * c}
    bar = pltpu.get_barrier_semaphore()
    for dev in (y_dev, c_dev, x_dev, xc_dev, yc_dev):
        pl.semaphore_signal(bar, inc=1, device_id=dev, device_id_type=MESH)

    def expert_load(j, e, with_q):
        m_buf, g_buf, q_buf = (mk.at[j], gk.at[j], qk.at[j]) if j < 2 else (md, gd, qd)
        copies = [pltpu.make_async_copy(em[j].at[e], m_buf, ld.at[j, 0]),
                  pltpu.make_async_copy(eg[j].at[e], g_buf, ld.at[j, 1])]
        if with_q:
            copies.append(pltpu.make_async_copy(eq[j].at[e], q_buf, ld.at[j, 2]))
        return copies

    def start_all(copies):
        for cp in copies:
            cp.start()

    def wait_all(copies):
        for cp in copies:
            cp.wait()

    def dense_load(i, s):
        slot = lax.rem(s, 2)
        rows = pl.ds(pl.multiple_of(slot * 256, 256), 256)
        return [pltpu.make_async_copy(dm[i].at[rows], mw.at[slot], ldw.at[slot, 0]),
                pltpu.make_async_copy(dg[i].at[rows], gw.at[slot], ldw.at[slot, 1])]

    def dense_q(i, s):
        slot = lax.rem(s // 2, 2)
        return pltpu.make_async_copy(dq[i], qw.at[slot], ldq.at[slot])

    def dense_start(s, with_q):
        for i in range(4):
            @pl.when(s // 2 == i)
            def _():
                start_all(dense_load(i, s))
        if with_q:
            for i in range(4):
                @pl.when(jnp.logical_and(s // 2 == i, lax.rem(s, 2) == 0))
                def _():
                    dense_q(i, s).start()

    def send(src, dst, kind, e, dev):
        return pltpu.make_async_remote_copy(src_ref=src, dst_ref=dst, send_sem=remote.at[0, kind, e],
                                            recv_sem=remote.at[1, kind, e], device_id=dev, device_id_type=MESH)

    def send_w(src, dst, kind, i, dev):
        return pltpu.make_async_remote_copy(src_ref=src, dst_ref=dst, send_sem=remote_w.at[0, kind, i],
                                            recv_sem=remote_w.at[1, kind, i], device_id=dev, device_id_type=MESH)

    def send_n(dst, kind, dev):
        return pltpu.make_async_remote_copy(src_ref=nrm, dst_ref=dst, send_sem=remote_n.at[0, kind],
                                            recv_sem=remote_n.at[1, kind], device_id=dev, device_id_type=MESH)

    def r_pk(e, j):
        return send(pk.at[e, j], pk_in.at[e, j], j, e, y_dev)

    def r_pd_c(e):
        return send(pd.at[e, 1 - c], pd_c.at[e], 2, e, c_dev)

    def r_pd_x(e):
        return send(pd.at[e, c], pd_x.at[e], 3, e, x_dev)

    def r_pd_o(e):
        return send(pf.at[e, c], pf.at[e, c], 4, e, c_dev)

    def r_sk_c(e):
        return send(sk.at[e, 1 - c], sk_c.at[e], 5, e, c_dev)

    def r_sk_x(e):
        return send(sk.at[e, c], sk_x.at[e], 6, e, x_dev)

    def r_sk_o(e):
        return send(sf.at[e, c], sf.at[e, c], 7, e, c_dev)

    def r_sd(e):
        return send(sd.at[e], sd_in.at[e, :, 0:384], 8, e, y_dev)

    def r_wd(e):
        return send(wd.at[e], wd_in.at[e], 9, e, y_dev)

    def r_pw(i):
        return send_w(pw.at[i], pw_in.at[i], 0, i, y_dev)

    def r_sw_c(d):
        return send_w(sw.at[2 * d + 1 - c], sw_c.at[d], 1, d, c_dev)

    def r_sw_x(d):
        return send_w(sw.at[2 * d + c], sw_x.at[d], 2, d, x_dev)

    def r_sw_o(d):
        return send_w(sfw.at[2 * d + c], sfw.at[2 * d + c], 3, d, c_dev)

    def out_pk(e):
        return pltpu.make_async_copy(pk_in.at[e], o_pk.at[e], out_sem.at[0, e])

    def out_pf(e):
        return pltpu.make_async_copy(pf.at[e], o_pf.at[e], out_sem.at[1, e])

    def out_sf(e, j):
        return pltpu.make_async_copy(sf.at[e, j], o_sf.at[e, j], out_sem.at[2 + j, e])

    def out_sd(e):
        return pltpu.make_async_copy(sd_in.at[e], o_sd.at[e], out_sem.at[4, e])

    def out_pw(i):
        return pltpu.make_async_copy(pw_in.at[i], o_pd.at[i], outw_sem.at[0, i])

    def out_sfw(i):
        return pltpu.make_async_copy(sfw.at[i], o_sfd.at[i], outw_sem.at[1, i])

    def block(j):
        if j < 2:
            return mk[j] + gk[j].astype(F32)
        return md[...] + gd[...].astype(F32)

    dense_start(0, True)
    for j in range(3):
        start_all(expert_load(j, 0, True))
    pl.semaphore_wait(bar, 5)

    def dense_one(s, carry):
        slot = lax.rem(s, 2)
        i = s // 2

        @pl.when(s < 7)
        def _():
            dense_start(s + 1, True)
        wait_all(dense_load(0, s))

        @pl.when(slot == 0)
        def _():
            dense_q(0, s).wait()
        b = mw[slot] + gw[slot].astype(F32)
        cols = pl.ds(pl.multiple_of(slot * 256, 256), 256)
        pw[i, :, cols] = dot6(qw[lax.rem(i, 2)].T, b, NT)

        @pl.when(slot == 1)
        def _():
            r_pw(i).start()
        return carry

    lax.fori_loop(0, 8, dense_one, 0)

    def pd_mid(e):
        r_pd_c(e).wait_recv()
        pd[e, c] = pd[e, c] + pd_c[e]
        r_pd_x(e).start()

    def expert_one(e, carry):
        for j in (2, 0, 1):
            wait_all(expert_load(j, e, True))
            q = qk[j] if j < 2 else qd[...]
            part = dot6(q, block(j), NN)

            @pl.when(e < 7)
            def _(j=j):
                start_all(expert_load(j, e + 1, True))
            if j < 2:
                pk[e, j] = part
                r_pk(e, j).start()
            else:
                pd[e, 0] = part[:, :512]
                pd[e, 1] = part[:, 512:]
                r_pd_c(e).start()
        pd_mid(e)
        return carry

    lax.fori_loop(0, 8, expert_one, 0)
    dense_start(0, False)
    for j in range(3):
        start_all(expert_load(j, 0, False))

    def dense_two(s, carry):
        slot = lax.rem(s, 2)
        i = s // 2

        @pl.when(s < 7)
        def _():
            dense_start(s + 1, False)

        @pl.when(slot == 0)
        def _():
            r_pw(i).wait_recv()
            total = pw[i] + pw_in[i]
            pw_in[i] = total
            out_pw(i).start()
            sw[i, :, 1024:] = dot6(total, total, NT)
            sw[i, :, :1024] = jnp.zeros((128, 1024), F32)
        wait_all(dense_load(0, s))
        b = mw[slot] + gw[slot].astype(F32)
        cols = pl.ds(pl.multiple_of(slot * 256, 256), 256)
        sw[i, :, :1024] = sw[i, :, :1024] + dot6(pw_in[i, :, cols], b, NN)

        @pl.when(lax.rem(s, 4) == 3)
        def _():
            r_sw_c(s // 4).start()
        return carry

    lax.fori_loop(0, 8, dense_two, 0)
    for d in range(2):
        r_sw_c(d).wait_recv()
        sw[2 * d + c] = sw[2 * d + c] + sw_c[d]
        r_sw_x(d).start()

    def down_two(s, carry):
        @pl.when(s < 8)
        def _():
            r_pd_x(s).wait_recv()
            pf[s, c] = pd[s, c] + pd_x[s]
            r_pd_o(s).start()

        @pl.when(s > 0)
        def _():
            e = s - 1
            r_pd_o(e).wait_recv()
            out_pf(e).start()
            wait_all(expert_load(2, e, False))
            total = jnp.concatenate([pf[e, 0], pf[e, 1]], axis=1)
            wd[e] = dot6(total, rows_to(total, 128), NT)
            r_wd(e).start()
            sd[e] = dot6(total, rows_to(block(2), 384), NT)

            @pl.when(e < 7)
            def _():
                start_all(expert_load(2, e + 1, False))
        return carry

    lax.fori_loop(0, 9, down_two, 0)

    def sd_send(e, carry):
        r_sd(e).start()
        return carry

    lax.fori_loop(0, 8, sd_send, 0)

    def keep_two(e, carry):
        for j in range(2):
            r_pk(e, j).wait_recv()
            total = pk[e, j] + pk_in[e, j]
            pk_in[e, j] = total
            wait_all(expert_load(j, e, False))
            sk[e, j, :, 768:] = dot6(total, rows_to(total, 128), NT)
            sk[e, j, :, :768] = dot6(total, rows_to(block(j), 768), NT)

            @pl.when(e < 7)
            def _(j=j):
                start_all(expert_load(j, e + 1, False))
        r_sk_c(e).start()
        out_pk(e).start()
        r_sk_c(e).wait_recv()
        sk[e, c] = sk[e, c] + sk_c[e]
        r_sk_x(e).start()
        return carry

    nrm[...] = jnp.zeros((128, LANES), F32)
    lane_full = lax.broadcasted_iota(jnp.int32, (128, LANES), 1)

    def add_norm(rt, where):
        sq = rows_to(jnp.sum(rt * rt, axis=1, keepdims=True), 128)
        nrm[...] = jnp.where(lane_full == where, sq, nrm[...])

    lax.fori_loop(0, 4, keep_two, 0)

    for d in range(2):
        r_sw_x(d).wait_recv()
        sfw[2 * d + c] = sw[2 * d + c] + sw_x[d]
    for s in range(8):
        aw[:, s, :] = sfw[2 * (s % 2) + c, :, 1024:]
    eliminate(aw, lw, 128)
    for d in range(2):
        i = 2 * d + c
        inv = lw[:, d, :]
        sfw[i, :, 1024:] = inv
        rt = dot6(inv, sfw[i, :, :1024], NN)
        sfw[i, :, :1024] = rt
        add_norm(rt, 24 + i)
        r_sw_o(d).start()

    lax.fori_loop(4, 8, keep_two, 0)

    for e in range(8):
        r_wd(e).wait_recv()
        ae[:, e, :] = wd[e] + wd_in[e]
    eliminate(ae, li, 88)
    for e in range(8):
        sd_in[e, :, 384:] = li[:, e, :]

    def keep_total(e, carry):
        r_sk_x(e).wait_recv()
        sf[e, c] = sk[e, c] + sk_x[e]
        return carry

    lax.fori_loop(0, 8, keep_total, 0)
    for e in range(8):
        ae[:, e, :] = sf[e, c, :, 768:]
    eliminate(ae, li, 88)
    for e in range(8):
        sf[e, c, :, 768:] = li[:, e, :]

    def keep_r(e, carry):
        rt = dot6(sf[e, c, :, 768:], rows_to(sf[e, c, :, :768], 128), NN)
        sf[e, c, :, :768] = rt
        add_norm(rt, 8 * c + e)
        r_sk_o(e).start()
        out_sf(e, c).start()
        return carry

    lax.fori_loop(0, 8, keep_r, 0)

    def down_r(e, carry):
        r_sd(e).wait_recv()
        st = sd[e] + sd_in[e, :, :384]
        rt = dot6(sd_in[e, :, 384:], rows_to(st, 128), NN)
        sd_in[e, :, :384] = rt
        add_norm(rt, 16 + e)
        out_sd(e).start()
        return carry

    lax.fori_loop(0, 8, down_r, 0)

    copies = [send_n(nrm_y, 0, y_dev), send_n(nrm_d, 1, yc_dev)]
    for k in range(1, 4):
        copies.append(send_n(nrm_f.at[k - 1], k + 1, {'fsdp': lax.rem(f + k, 4)}))
    start_all(copies)

    def finish(e, carry):
        r_sk_o(e).wait_recv()
        out_sf(e, 1 - c).start()
        return carry

    lax.fori_loop(0, 8, finish, 0)
    for d in range(2):
        out_sfw(2 * d + c).start()
        r_sw_o(d).wait_recv()
        out_sfw(2 * d + 1 - c).start()
    wait_all(copies)
    own = nrm[...]
    over_f = jnp.zeros((128, LANES), F32)
    for dev in range(4):
        k = lax.rem(f - dev + 4, 4)
        over_f = over_f + jnp.where(k == 0, own, jnp.where(k == 1, nrm_f[0], jnp.where(k == 2, nrm_f[1], nrm_f[2])))
    core = jnp.where(c == 0, nrm_f[2], nrm_f[0])
    owner = jnp.where(lane_full < 24, lane_full // 8, lax.rem(lane_full, 2))
    keep = jnp.where(owner == c, own + nrm_y[...], core + nrm_d[...])
    is_down = jnp.logical_and(lane_full >= 16, lane_full < 24)
    total = jnp.where(is_down, over_f, keep)
    nrm[...] = 1.0 / jnp.sqrt(total)
    last = pltpu.make_async_copy(nrm, o_nrm, outw_sem.at[0, 4])
    last.start()

    def drain(e, carry):
        for r in (r_pk(e, 0), r_pk(e, 1), r_pd_c(e), r_pd_x(e), r_pd_o(e), r_sk_c(e), r_sk_x(e), r_sk_o(e), r_sd(e), r_wd(e)):
            r.wait_send()
        for o in (out_pk(e), out_pf(e), out_sf(e, 0), out_sf(e, 1), out_sd(e)):
            o.wait()
        return carry

    lax.fori_loop(0, 8, drain, 0)
    for i in range(4):
        r_pw(i).wait_send()
        out_pw(i).wait()
        out_sfw(i).wait()
    for d in range(2):
        r_sw_c(d).wait_send()
        r_sw_x(d).wait_send()
        r_sw_o(d).wait_send()
    last.wait()


def exchange(experts, dense):
    any_spec = pl.BlockSpec(memory_space=pl.ANY)
    args = [a for grp in experts for a in grp] + [a for grp in dense for a in grp]
    shapes = [(8, 2, 88, 512), (8, 2, 88, 512), (8, 2, 88, 896), (8, 88, 512), (4, 128, 512), (4, 128, 1152), (128, 128)]
    dma = pltpu.SemaphoreType.DMA

    def v(*shape, dtype=F32):
        return pltpu.VMEM(shape, dtype)

    scratch = [v(2, 704, 512), v(2, 704, 512, dtype=BF), v(2, 88, 704),
               v(352, 1024), v(352, 1024, dtype=BF), v(88, 352),
               v(2, 256, 1024), v(2, 256, 1024, dtype=BF), v(2, 1024, 128),
               v(8, 2, 88, 512), v(8, 2, 88, 512),
               v(8, 2, 88, 512), v(8, 88, 512), v(8, 88, 512), v(8, 2, 88, 512),
               v(8, 2, 88, 896), v(8, 88, 896), v(8, 88, 896), v(8, 2, 88, 896),
               v(8, 88, 384), v(8, 88, 512), v(8, 88, 128), v(8, 88, 128),
               v(4, 128, 512), v(4, 128, 512), v(4, 128, 1152), v(2, 128, 1152), v(2, 128, 1152), v(4, 128, 1152),
               v(88, 8, 128), v(88, 8, 128), v(128, 8, 128), v(128, 8, 128),
               v(128, 128), v(128, 128), v(128, 128), v(3, 128, 128),
               dma((3, 3)), dma((2, 2)), dma((2,)), dma((5, 8)), dma((2, 5)), dma((2, 10, 8)), dma((2, 4, 4)), dma((2, 5))]
    return pl.pallas_call(
        exchange_kernel,
        in_specs=[any_spec] * len(args), out_specs=[any_spec] * len(shapes),
        out_shape=[jax.ShapeDtypeStruct(s, F32) for s in shapes],
        scratch_shapes=scratch,
        compiler_params=pltpu.CompilerParams(collective_id=0, has_side_effects=True, vmem_limit_bytes=67043328),
        name='exchange',
    )(*args)


def left_cat(ut):
    h, m, l = split3(rows_to(ut, LANES).T)
    return jnp.concatenate([h, l, m, m, h, h], axis=1)


def right_cat(vt):
    h, m, l = split3(rows_to(vt, LANES))
    return jnp.concatenate([l, h, m, h, m, h], axis=0)


def take_col(dinv_ref, rank, where):
    lane = lax.broadcasted_iota(jnp.int32, (rank, LANES), 1)
    return jnp.sum(jnp.where(lane == where, dinv_ref[:rank, :], 0.0), axis=1, keepdims=True)


def apply_update(x_ref, m_ref, g_ref, ut, vt, dinv, x_out, m_out, scale):
    left = left_cat(ut)
    b = m_ref[...] + g_ref[...].astype(F32)
    m_out[...] = b - (1.0 - MOMENTUM) * jnp.dot(left, right_cat(vt), preferred_element_type=F32)
    x_out[...] = x_ref[...] - scale * jnp.dot(left, right_cat(vt * dinv), preferred_element_type=F32)


def expert_kernel(*refs):
    e = pl.program_id(0)
    pk, pf, sf, sd, dinv_ref = refs[9:14]
    scale = LEARN_RATE * math.sqrt(2048 / 1408)
    for j in range(3):
        x_ref, m_ref, g_ref = (r.at[0] for r in refs[3 * j:3 * j + 3])
        x_out, m_out, q_out = (r.at[0] for r in refs[14 + 3 * j:17 + 3 * j])
        dinv = take_col(dinv_ref, 88, 8 * j + e)
        if j < 2:
            pt, rt, inv = pk[0, j], sf[0, j, :, :704], sf[0, j, :, 768:]
        else:
            pt, rt, inv = jnp.concatenate([pf[0, 0], pf[0, 1]], axis=1), sd[0, :, :352], sd[0, :, 384:]
        pt = dot6(inv, rows_to(pt, LANES), NN)
        apply_update(x_ref, m_ref, g_ref, rt, pt, dinv, x_out, m_out, scale)
        q_out[...] = rt * dinv


def expert_update(mats, sums):
    def blk(a):
        n = len(a.shape)
        return pl.BlockSpec((1,) + a.shape[1:], lambda e: (e,) + (0,) * (n - 1))

    args = [a for grp in mats for a in grp] + list(sums)
    in_specs = [blk(a) for a in args[:-1]] + [pl.BlockSpec((128, 128), lambda e: (0, 0))]
    out_shape = []
    for x, _, _ in mats:
        q_shape = (8, 88, x.shape[1])
        out_shape += [jax.ShapeDtypeStruct(s, F32) for s in (x.shape, x.shape, q_shape)]
    return pl.pallas_call(
        expert_kernel, grid=(8,), in_specs=in_specs, out_specs=[blk(o) for o in out_shape], out_shape=out_shape,
        compiler_params=pltpu.CompilerParams(vmem_limit_bytes=62 * MIB),
        name='expert_update',
    )(*args)


DENSE_STEPS = 4


def dense_kernel(*refs):
    pw, sfw, dinv_ref = refs[12:15]
    part = pl.program_id(0)
    for i in range(4):
        x_ref, m_ref, g_ref = refs[3 * i:3 * i + 3]
        x_out, m_out, q_out = refs[15 + 3 * i:18 + 3 * i]
        dinv = take_col(dinv_ref, 128, 24 + i)
        pt = dot6(sfw[i, :, 1024:], pw[i], NN)
        apply_update(x_ref, m_ref, g_ref, pt, sfw[i, :, :1024], dinv, x_out, m_out, LEARN_RATE)
        q_rows = q_out.shape[0]
        q_out[...] = (sfw[i, :, pl.ds(pl.multiple_of(part * q_rows, q_rows), q_rows)] * dinv).T


def dense_update(mats, pw, sfw, dinv):
    args = [a for grp in mats for a in grp] + [pw, sfw, dinv]
    rows, cols = mats[0][0].shape
    blk = pl.BlockSpec((rows // DENSE_STEPS, cols), lambda s: (s, 0))
    q_blk = pl.BlockSpec((cols // DENSE_STEPS, 128), lambda s: (s, 0))
    in_specs = [blk] * 12 + [pl.BlockSpec((4, 128, rows // DENSE_STEPS), lambda s: (0, 0, s)),
                             pl.BlockSpec(sfw.shape, lambda s: (0, 0, 0)),
                             pl.BlockSpec(dinv.shape, lambda s: (0, 0))]
    w_out = jax.ShapeDtypeStruct((rows, cols), F32)
    return pl.pallas_call(
        dense_kernel, grid=(DENSE_STEPS,), in_specs=in_specs, out_specs=[blk, blk, q_blk] * 4,
        out_shape=[w_out, w_out, jax.ShapeDtypeStruct((cols, 128), F32)] * 4,
        compiler_params=pltpu.CompilerParams(vmem_limit_bytes=60 * MIB),
        name='dense_update',
    )(*args)


def solution(mesh):
    dense_w = P(('layer', 'fsdp'), 'tp')
    dense_f = P(('layer', 'tp'), None)
    stack_w = P('layer', 'fsdp', 'tp')
    stack_f = P('layer', 'tp', None)
    down_f = P('layer', 'fsdp', None)
    in_specs = (dense_w, dense_w, dense_w, dense_f) * 4 + (stack_w, stack_w, stack_w, stack_f) * 2 + (stack_w, stack_w, stack_w, down_f)
    out_specs = (dense_w, dense_w, dense_f) * 4 + (stack_w, stack_w, stack_f) * 2 + (stack_w, stack_w, down_f)

    def local_step(*blocks):
        dense = [blocks[4 * i:4 * i + 4] for i in range(4)]
        experts = []
        for i in (4, 5, 6):
            w, m, g, q = blocks[4 * i:4 * i + 4]
            if i < 6:
                w, m, g = (a.swapaxes(1, 2) for a in (w, m, g))
            experts.append((w, m, g, q.swapaxes(1, 2)))
        pk, pf, sf, sd, pw, sfw, dinv = exchange([grp[1:] for grp in experts], [grp[1:] for grp in dense])
        results = list(dense_update([grp[:3] for grp in dense], pw, sfw, dinv))
        out = list(expert_update([grp[:3] for grp in experts], (pk, pf, sf, sd, dinv)))
        for n in range(9):
            if n < 6 or n == 8:
                out[n] = out[n].swapaxes(1, 2)
        return tuple(results + out)

    return jax.shard_map(local_step, mesh=mesh, in_specs=in_specs, out_specs=out_specs, check_vma=False)
```

```python
import math
import jax
import jax.numpy as jnp
from jax import lax
from jax.experimental import pallas as pl
from jax.experimental.pallas import tpu as pltpu
from jax.sharding import PartitionSpec as P

MOMENTUM = 0.9
LEARN_RATE = 0.3
LANES = 128
BF = jnp.bfloat16
F32 = jnp.float32
MIB = 2 ** 20
NN = (((1,), (0,)), ((), ()))
NT = (((1,), (1,)), ((), ()))
MESH = pl.DeviceIdType.MESH


def split3(x):
    hi = x.astype(BF)
    rest = x - hi.astype(F32)
    mid = rest.astype(BF)
    low = (rest - mid.astype(F32)).astype(BF)
    return hi, mid, low


def rows_to(x, rows):
    have, cols = x.shape
    if have == rows:
        return x
    return jnp.concatenate([x, jnp.zeros((rows - have, cols), x.dtype)], axis=0)


def dot6(left, right, dims):
    rank = left.shape[0]
    pad = -(-rank // 16) * 16
    lh, lm, ll = split3(rows_to(left, pad))
    rh, rm, rl = split3(right)
    with_h = lax.dot_general(jnp.concatenate([lh, lm, ll], axis=0), rh, dims, preferred_element_type=F32)
    with_m = lax.dot_general(jnp.concatenate([lh, lm], axis=0), rm, dims, preferred_element_type=F32)
    with_l = lax.dot_general(lh, rl, dims, preferred_element_type=F32)
    small = with_h[2 * pad:2 * pad + rank] + with_m[pad:pad + rank] + with_l[:rank]
    mid = with_h[pad:pad + rank] + with_m[:rank]
    return (small + mid) + with_h[:rank]


def eliminate(a, li, rank):
    lane = lax.broadcasted_iota(jnp.int32, (8, LANES), 1)

    def pick(x, hit):
        return jnp.sum(jnp.where(hit, x, 0.0), axis=-1, keepdims=True)

    for k0 in range(0, rank, 8):
        def step(kk, carry, k0=k0):
            k = k0 + 2 * kk
            h0, h1 = lane == k, lane == k + 1
            r0, r1 = a[k], a[k + 1]
            v00, v01, v10, v11 = pick(r0, h0), pick(r0, h1), pick(r1, h0), pick(r1, h1)
            rinv0 = 1.0 / v00
            rs0 = 1.0 / jnp.sqrt(v00)
            s01 = v01 * rinv0
            sc0 = jnp.where(h0, rinv0, r0 * rinv0)
            li[k] = jnp.where(h0, rs0, jnp.where(lane < k, r0 * rs0, 0.0))
            piv1 = v11 - v10 * s01
            rinv1 = 1.0 / piv1
            rs1 = 1.0 / jnp.sqrt(piv1)
            r1 = jnp.where(h0, 0.0, r1) - v10 * sc0
            sc1 = jnp.where(h1, rinv1, r1 * rinv1)
            li[k + 1] = jnp.where(h1, rs1, jnp.where(lane < k + 1, r1 * rs1, 0.0))
            sc0 = jnp.where(h1, 0.0, sc0)

            def below(lo, n, masked):
                lane_n = lax.broadcasted_iota(jnp.int32, (n, 8, LANES), 2)
                g_hit0, g_hit1 = lane_n == k, lane_n == k + 1
                cur = a[lo:lo + n]
                g0 = pick(cur, g_hit0)
                g1 = pick(cur, g_hit1) - g0 * s01[None]
                new = jnp.where(jnp.logical_or(g_hit0, g_hit1), 0.0, cur) - g0 * sc0[None] - g1 * sc1[None]
                if masked:
                    row = lo + lax.broadcasted_iota(jnp.int32, (n, 8, LANES), 0)
                    new = jnp.where(row > k + 1, new, cur)
                a[lo:lo + n] = new

            below(k0, 8, True)
            if rank > k0 + 8:
                below(k0 + 8, rank - k0 - 8, False)
            return carry
        lax.fori_loop(0, 4, step, 0)


def exchange_kernel(*refs):
    em, eg, eq = refs[0:9:3], refs[1:9:3], refs[2:9:3]
    dm, dg, dq = refs[9:21:3], refs[10:21:3], refs[11:21:3]
    o_pk, o_pf, o_sf, o_sd, o_pd, o_sfd, o_nrm = refs[21:28]
    (mk, gk, qk, md, gd, qd, mw, gw, qw,
     pk, pk_in, pd, pd_c, pd_x, pf, sk, sk_c, sk_x, sk_o, wk, wk_c, wk_x, sd, sd_in, wd, wd_in,
     pw, pw_in, sw, sw_c, sw_x, sfw, ae, li, aw, lw, nrm, nrm_y, nrm_d, nrm_f,
     ld, ldw, ldq, out_sem, outw_sem, remote, remote_w, remote_n) = refs[28:]
    t = lax.axis_index('tp')
    f = lax.axis_index('fsdp')
    c = lax.rem(f, 2)
    y_dev = {'tp': 1 - t}
    c_dev = {'fsdp': f + 1 - 2 * c}
    x_dev = {'fsdp': lax.rem(f + 2, 4)}
    xc_dev = {'fsdp': lax.rem(f + 3 - 2 * c, 4)}
    yc_dev = {'tp': 1 - t, 'fsdp': f + 1 - 2 * c}
    bar = pltpu.get_barrier_semaphore()
    for dev in (y_dev, c_dev, x_dev, xc_dev, yc_dev):
        pl.semaphore_signal(bar, inc=1, device_id=dev, device_id_type=MESH)

    def expert_load(j, e, with_q):
        m_buf, g_buf, q_buf = (mk.at[j], gk.at[j], qk.at[j]) if j < 2 else (md, gd, qd)
        slot = lax.rem(e, 2)
        m_buf, g_buf, q_buf = m_buf.at[slot], g_buf.at[slot], q_buf.at[slot]
        copies = [pltpu.make_async_copy(em[j].at[e], m_buf, ld.at[j, 0, slot]),
                  pltpu.make_async_copy(eg[j].at[e], g_buf, ld.at[j, 1, slot])]
        if with_q:
            copies.append(pltpu.make_async_copy(eq[j].at[e], q_buf, ld.at[j, 2, slot]))
        return copies

    def start_all(copies):
        for cp in copies:
            cp.start()

    def wait_all(copies):
        for cp in copies:
            cp.wait()

    def dense_load(i, s):
        slot = lax.rem(s, 2)
        rows = pl.ds(pl.multiple_of(slot * 256, 256), 256)
        return [pltpu.make_async_copy(dm[i].at[rows], mw.at[slot], ldw.at[slot, 0]),
                pltpu.make_async_copy(dg[i].at[rows], gw.at[slot], ldw.at[slot, 1])]

    def dense_q(i, s):
        slot = lax.rem(s // 2, 2)
        return pltpu.make_async_copy(dq[i], qw.at[slot], ldq.at[slot])

    def dense_start(s, with_q):
        for i in range(4):
            @pl.when(s // 2 == i)
            def _():
                start_all(dense_load(i, s))
        if with_q:
            for i in range(4):
                @pl.when(jnp.logical_and(s // 2 == i, lax.rem(s, 2) == 0))
                def _():
                    dense_q(i, s).start()

    def send(src, dst, kind, e, dev):
        return pltpu.make_async_remote_copy(src_ref=src, dst_ref=dst, send_sem=remote.at[0, kind, e],
                                            recv_sem=remote.at[1, kind, e], device_id=dev, device_id_type=MESH)

    def send_w(src, dst, kind, i, dev):
        return pltpu.make_async_remote_copy(src_ref=src, dst_ref=dst, send_sem=remote_w.at[0, kind, i],
                                            recv_sem=remote_w.at[1, kind, i], device_id=dev, device_id_type=MESH)

    def send_n(dst, kind, dev):
        return pltpu.make_async_remote_copy(src_ref=nrm, dst_ref=dst, send_sem=remote_n.at[0, kind],
                                            recv_sem=remote_n.at[1, kind], device_id=dev, device_id_type=MESH)

    def r_pk(e, j):
        return send(pk.at[e, j], pk_in.at[e, j], j, e, y_dev)

    def r_pd_c(e):
        return send(pd.at[e, 1 - c], pd_c.at[e], 2, e, c_dev)

    def r_pd_x(e):
        return send(pd.at[e, c], pd_x.at[e], 3, e, x_dev)

    def r_pd_o(e):
        return send(pf.at[e, c], pf.at[e, c], 4, e, c_dev)

    def r_sk_c(e):
        return send(sk.at[e, 1 - c], sk_c.at[e], 5, e, c_dev)

    def r_sk_x(e):
        return send(sk.at[e, c], sk_x.at[e, :, 0:768], 6, e, x_dev)

    def r_sk_o(e):
        return send(sk_x.at[e], sk_o.at[e], 7, e, c_dev)

    def r_wk_c(e):
        return send(wk.at[e, 1 - c], wk_c.at[e], 10, e, c_dev)

    def r_wk_x(e):
        return send(wk.at[e, c], wk_x.at[e], 11, e, x_dev)

    def r_sd(e):
        return send(sd.at[e], sd_in.at[e, :, 0:384], 8, e, y_dev)

    def r_wd(e):
        return send(wd.at[e], wd_in.at[e], 9, e, y_dev)

    def r_pw(i):
        return send_w(pw.at[i], pw_in.at[i], 0, i, y_dev)

    def r_sw_c(d):
        return send_w(sw.at[2 * d + 1 - c], sw_c.at[d], 1, d, c_dev)

    def r_sw_x(d):
        return send_w(sw.at[2 * d + c], sw_x.at[d], 2, d, x_dev)

    def r_sw_o(d):
        return send_w(sfw.at[2 * d + c], sfw.at[2 * d + c], 3, d, c_dev)

    def out_pk(e):
        return pltpu.make_async_copy(pk_in.at[e], o_pk.at[e], out_sem.at[0, e])

    def out_pf(e):
        return pltpu.make_async_copy(pf.at[e], o_pf.at[e], out_sem.at[1, e])

    def out_own(e):
        return pltpu.make_async_copy(sk_x.at[e], o_sf.at[e, c], out_sem.at[2, e])

    def out_other(e):
        return pltpu.make_async_copy(sk_o.at[e], o_sf.at[e, 1 - c], out_sem.at[3, e])

    def out_sd(e):
        return pltpu.make_async_copy(sd_in.at[e], o_sd.at[e], out_sem.at[4, e])

    def out_pw(i):
        return pltpu.make_async_copy(pw_in.at[i], o_pd.at[i], outw_sem.at[0, i])

    def out_sfw(i):
        return pltpu.make_async_copy(sfw.at[i], o_sfd.at[i], outw_sem.at[1, i])

    def block(j, e):
        slot = lax.rem(e, 2)
        if j < 2:
            return mk[j, slot] + gk[j, slot].astype(F32)
        return md[slot] + gd[slot].astype(F32)

    for e in range(2):
        for j in (2, 0, 1):
            start_all(expert_load(j, e, True))
    dense_start(0, True)
    pl.semaphore_wait(bar, 5)

    def dense_one(s, carry):
        slot = lax.rem(s, 2)
        i = s // 2

        @pl.when(s < 7)
        def _():
            dense_start(s + 1, True)
        wait_all(dense_load(0, s))

        @pl.when(slot == 0)
        def _():
            dense_q(0, s).wait()
        b = mw[slot] + gw[slot].astype(F32)
        cols = pl.ds(pl.multiple_of(slot * 256, 256), 256)
        pw[i, :, cols] = dot6(qw[lax.rem(i, 2)].T, b, NT)

        @pl.when(slot == 1)
        def _():
            r_pw(i).start()
        return carry


    def pd_mid(e):
        r_pd_c(e).wait_recv()
        pd[e, c] = pd[e, c] + pd_c[e]
        r_pd_x(e).start()

    def expert_one(e, carry):
        for j in (2, 0, 1):
            wait_all(expert_load(j, e, True))
            slot = lax.rem(e, 2)
            q = qk[j, slot] if j < 2 else qd[slot]
            part = dot6(q, block(j, e), NN)

            @pl.when(e < 6)
            def _(j=j):
                start_all(expert_load(j, e + 2, True))
            if j < 2:
                pk[e, j] = part
                r_pk(e, j).start()
            else:
                pd[e, 0] = part[:, :512]
                pd[e, 1] = part[:, 512:]
                r_pd_c(e).start()
        pd_mid(e)
        return carry

    lax.fori_loop(0, 2, expert_one, 0)
    lax.fori_loop(0, 8, dense_one, 0)
    lax.fori_loop(2, 8, expert_one, 0)
    for e in range(2):
        for j in range(3):
            start_all(expert_load(j, e, False))
    dense_start(0, False)

    def dense_two(s, carry):
        slot = lax.rem(s, 2)
        i = s // 2

        @pl.when(s < 7)
        def _():
            dense_start(s + 1, False)

        @pl.when(slot == 0)
        def _():
            r_pw(i).wait_recv()
            total = pw[i] + pw_in[i]
            pw_in[i] = total
            out_pw(i).start()
            sw[i, :, 1024:] = dot6(total, total, NT)
            sw[i, :, :1024] = jnp.zeros((128, 1024), F32)
        wait_all(dense_load(0, s))
        b = mw[slot] + gw[slot].astype(F32)
        cols = pl.ds(pl.multiple_of(slot * 256, 256), 256)
        sw[i, :, :1024] = sw[i, :, :1024] + dot6(pw_in[i, :, cols], b, NN)

        @pl.when(lax.rem(s, 4) == 3)
        def _():
            r_sw_c(s // 4).start()
        return carry

    def down_two(s, carry):
        @pl.when(s < 8)
        def _():
            r_pd_x(s).wait_recv()
            pf[s, c] = pd[s, c] + pd_x[s]
            r_pd_o(s).start()

        @pl.when(s > 0)
        def _():
            e = s - 1
            r_pd_o(e).wait_recv()
            out_pf(e).start()
            wait_all(expert_load(2, e, False))
            total = jnp.concatenate([pf[e, 0], pf[e, 1]], axis=1)
            wd[e] = dot6(total, rows_to(total, 128), NT)
            r_wd(e).start()
            sd[e] = dot6(total, rows_to(block(2, e), 384), NT)

            @pl.when(e < 6)
            def _():
                start_all(expert_load(2, e + 2, False))
        return carry

    def sd_send(e, carry):
        r_sd(e).start()
        return carry

    def sk_mid(e):
        r_sk_c(e).wait_recv()
        sk[e, c] = sk[e, c] + sk_c[e]
        r_sk_x(e).start()

    def keep_two(e, carry):
        for j in range(2):
            r_pk(e, j).wait_recv()
            total = pk[e, j] + pk_in[e, j]
            pk_in[e, j] = total
            wk[e, j] = dot6(total, rows_to(total, 128), NT)
        r_wk_c(e).start()
        out_pk(e).start()
        for j in range(2):
            wait_all(expert_load(j, e, False))
            sk[e, j] = dot6(pk_in[e, j], rows_to(block(j, e), 768), NT)

            @pl.when(e < 6)
            def _(j=j):
                start_all(expert_load(j, e + 2, False))
        r_sk_c(e).start()
        r_wk_c(e).wait_recv()
        wk[e, c] = wk[e, c] + wk_c[e]
        r_wk_x(e).start()

        @pl.when(e > 3)
        def _():
            sk_mid(e - 2)
        return carry

    lax.fori_loop(0, 2, keep_two, 0)
    sk_mid(0)
    sk_mid(1)
    lax.fori_loop(0, 9, down_two, 0)
    lax.fori_loop(0, 8, sd_send, 0)
    lax.fori_loop(0, 8, dense_two, 0)
    for d in range(2):
        r_sw_c(d).wait_recv()
        sw[2 * d + c] = sw[2 * d + c] + sw_c[d]
        r_sw_x(d).start()


    nrm[...] = jnp.zeros((128, LANES), F32)
    lane_full = lax.broadcasted_iota(jnp.int32, (128, LANES), 1)

    def add_norm(rt, where):
        sq = rows_to(jnp.sum(rt * rt, axis=1, keepdims=True), 128)
        nrm[...] = jnp.where(lane_full == where, sq, nrm[...])

    lax.fori_loop(2, 6, keep_two, 0)

    for d in range(2):
        r_sw_x(d).wait_recv()
        sfw[2 * d + c] = sw[2 * d + c] + sw_x[d]
    for s in range(8):
        aw[:, s, :] = sfw[2 * (s % 2) + c, :, 1024:]
    eliminate(aw, lw, 128)
    for d in range(2):
        i = 2 * d + c
        inv = lw[:, d, :]
        sfw[i, :, 1024:] = inv
        rt = dot6(inv, sfw[i, :, :1024], NN)
        sfw[i, :, :1024] = rt
        add_norm(rt, 24 + i)
        r_sw_o(d).start()

    lax.fori_loop(6, 8, keep_two, 0)
    sk_mid(6)
    sk_mid(7)

    for e in range(8):
        r_wd(e).wait_recv()
        ae[:, e, :] = wd[e] + wd_in[e]
    eliminate(ae, li, 88)
    for e in range(8):
        sd_in[e, :, 384:] = li[:, e, :]

    for e in range(8):
        r_wk_x(e).wait_recv()
        ae[:, e, :] = wk[e, c] + wk_x[e]
    eliminate(ae, li, 88)
    for e in range(8):
        sk_x[e, :, 768:] = li[:, e, :]

    def keep_r(e, carry):
        r_sk_x(e).wait_recv()
        st = sk[e, c] + sk_x[e, :, :768]
        rt = dot6(sk_x[e, :, 768:], rows_to(st, 128), NN)
        sk_x[e, :, :768] = rt
        r_sk_o(e).start()
        add_norm(rt, 8 * c + e)
        out_own(e).start()
        return carry

    lax.fori_loop(0, 8, keep_r, 0)

    def down_r(e, carry):
        r_sd(e).wait_recv()
        st = sd[e] + sd_in[e, :, :384]
        rt = dot6(sd_in[e, :, 384:], rows_to(st, 128), NN)
        sd_in[e, :, :384] = rt
        add_norm(rt, 16 + e)
        out_sd(e).start()
        return carry

    lax.fori_loop(0, 8, down_r, 0)

    copies = [send_n(nrm_y, 0, y_dev), send_n(nrm_d, 1, yc_dev)]
    for k in range(1, 4):
        copies.append(send_n(nrm_f.at[k - 1], k + 1, {'fsdp': lax.rem(f + k, 4)}))
    start_all(copies)

    def finish(e, carry):
        r_sk_o(e).wait_recv()
        out_other(e).start()
        return carry

    lax.fori_loop(0, 8, finish, 0)
    for d in range(2):
        out_sfw(2 * d + c).start()
        r_sw_o(d).wait_recv()
        out_sfw(2 * d + 1 - c).start()
    wait_all(copies)
    own = nrm[...]
    over_f = jnp.zeros((128, LANES), F32)
    for dev in range(4):
        k = lax.rem(f - dev + 4, 4)
        over_f = over_f + jnp.where(k == 0, own, jnp.where(k == 1, nrm_f[0], jnp.where(k == 2, nrm_f[1], nrm_f[2])))
    core = jnp.where(c == 0, nrm_f[2], nrm_f[0])
    owner = jnp.where(lane_full < 24, lane_full // 8, lax.rem(lane_full, 2))
    keep = jnp.where(owner == c, own + nrm_y[...], core + nrm_d[...])
    is_down = jnp.logical_and(lane_full >= 16, lane_full < 24)
    total = jnp.where(is_down, over_f, keep)
    nrm[...] = 1.0 / jnp.sqrt(total)
    last = pltpu.make_async_copy(nrm, o_nrm, outw_sem.at[0, 4])
    last.start()

    def drain(e, carry):
        for r in (r_pk(e, 0), r_pk(e, 1), r_pd_c(e), r_pd_x(e), r_pd_o(e), r_sk_c(e), r_sk_x(e), r_sk_o(e), r_sd(e), r_wd(e), r_wk_c(e), r_wk_x(e)):
            r.wait_send()
        for o in (out_pk(e), out_pf(e), out_own(e), out_other(e), out_sd(e)):
            o.wait()
        return carry

    lax.fori_loop(0, 8, drain, 0)
    for i in range(4):
        r_pw(i).wait_send()
        out_pw(i).wait()
        out_sfw(i).wait()
    for d in range(2):
        r_sw_c(d).wait_send()
        r_sw_x(d).wait_send()
        r_sw_o(d).wait_send()
    last.wait()


def exchange(experts, dense):
    any_spec = pl.BlockSpec(memory_space=pl.ANY)
    args = [a for grp in experts for a in grp] + [a for grp in dense for a in grp]
    shapes = [(8, 2, 88, 512), (8, 2, 88, 512), (8, 2, 88, 896), (8, 88, 512), (4, 128, 512), (4, 128, 1152), (128, 128)]
    dma = pltpu.SemaphoreType.DMA

    def v(*shape, dtype=F32):
        return pltpu.VMEM(shape, dtype)

    scratch = [v(2, 2, 704, 512), v(2, 2, 704, 512, dtype=BF), v(2, 2, 88, 704),
               v(2, 352, 1024), v(2, 352, 1024, dtype=BF), v(2, 88, 352),
               v(2, 256, 1024), v(2, 256, 1024, dtype=BF), v(2, 1024, 128),
               v(8, 2, 88, 512), v(8, 2, 88, 512),
               v(8, 2, 88, 512), v(8, 88, 512), v(8, 88, 512), v(8, 2, 88, 512),
               v(8, 2, 88, 768), v(8, 88, 768), v(8, 88, 896), v(8, 88, 896),
               v(8, 2, 88, 128), v(8, 88, 128), v(8, 88, 128),
               v(8, 88, 384), v(8, 88, 512), v(8, 88, 128), v(8, 88, 128),
               v(4, 128, 512), v(4, 128, 512), v(4, 128, 1152), v(2, 128, 1152), v(2, 128, 1152), v(4, 128, 1152),
               v(88, 8, 128), v(88, 8, 128), v(128, 8, 128), v(128, 8, 128),
               v(128, 128), v(128, 128), v(128, 128), v(3, 128, 128),
               dma((3, 3, 2)), dma((2, 2)), dma((2,)), dma((5, 8)), dma((2, 5)), dma((2, 12, 8)), dma((2, 4, 4)), dma((2, 5))]
    return pl.pallas_call(
        exchange_kernel,
        in_specs=[any_spec] * len(args), out_specs=[any_spec] * len(shapes),
        out_shape=[jax.ShapeDtypeStruct(s, F32) for s in shapes],
        scratch_shapes=scratch,
        compiler_params=pltpu.CompilerParams(collective_id=0, has_side_effects=True, vmem_limit_bytes=67043328),
        name='exchange',
    )(*args)


def left_cat(ut):
    h, m, l = split3(rows_to(ut, LANES).T)
    return jnp.concatenate([h, l, m, m, h, h], axis=1)


def right_cat(vt):
    h, m, l = split3(rows_to(vt, LANES))
    return jnp.concatenate([l, h, m, h, m, h], axis=0)


def take_col(dinv_ref, rank, where):
    lane = lax.broadcasted_iota(jnp.int32, (rank, LANES), 1)
    return jnp.sum(jnp.where(lane == where, dinv_ref[:rank, :], 0.0), axis=1, keepdims=True)


def apply_update(x_ref, m_ref, g_ref, ut, vt, dinv, x_out, m_out, scale):
    left = left_cat(ut)
    b = m_ref[...] + g_ref[...].astype(F32)
    m_out[...] = b - (1.0 - MOMENTUM) * jnp.dot(left, right_cat(vt), preferred_element_type=F32)
    x_out[...] = x_ref[...] - scale * jnp.dot(left, right_cat(vt * dinv), preferred_element_type=F32)


def expert_kernel(*refs):
    e = pl.program_id(0)
    pk, pf, sf, sd, dinv_ref = refs[9:14]
    scale = LEARN_RATE * math.sqrt(2048 / 1408)
    for j in range(3):
        x_ref, m_ref, g_ref = (r.at[0] for r in refs[3 * j:3 * j + 3])
        x_out, m_out, q_out = (r.at[0] for r in refs[14 + 3 * j:17 + 3 * j])
        dinv = take_col(dinv_ref, 88, 8 * j + e)
        if j < 2:
            pt, rt, inv = pk[0, j], sf[0, j, :, :704], sf[0, j, :, 768:]
        else:
            pt, rt, inv = jnp.concatenate([pf[0, 0], pf[0, 1]], axis=1), sd[0, :, :352], sd[0, :, 384:]
        pt = dot6(inv, rows_to(pt, LANES), NN)
        apply_update(x_ref, m_ref, g_ref, rt, pt, dinv, x_out, m_out, scale)
        q_out[...] = rt * dinv


def expert_update(mats, sums):
    def blk(a):
        n = len(a.shape)
        return pl.BlockSpec((1,) + a.shape[1:], lambda e: (e,) + (0,) * (n - 1))

    args = [a for grp in mats for a in grp] + list(sums)
    in_specs = [blk(a) for a in args[:-1]] + [pl.BlockSpec((128, 128), lambda e: (0, 0))]
    out_shape = []
    for x, _, _ in mats:
        q_shape = (8, 88, x.shape[1])
        out_shape += [jax.ShapeDtypeStruct(s, F32) for s in (x.shape, x.shape, q_shape)]
    return pl.pallas_call(
        expert_kernel, grid=(8,), in_specs=in_specs, out_specs=[blk(o) for o in out_shape], out_shape=out_shape,
        compiler_params=pltpu.CompilerParams(vmem_limit_bytes=62 * MIB),
        name='expert_update',
    )(*args)


DENSE_STEPS = 4


def dense_kernel(*refs):
    pw, sfw, dinv_ref = refs[12:15]
    part = pl.program_id(0)
    for i in range(4):
        x_ref, m_ref, g_ref = refs[3 * i:3 * i + 3]
        x_out, m_out, q_out = refs[15 + 3 * i:18 + 3 * i]
        dinv = take_col(dinv_ref, 128, 24 + i)
        pt = dot6(sfw[i, :, 1024:], pw[i], NN)
        apply_update(x_ref, m_ref, g_ref, pt, sfw[i, :, :1024], dinv, x_out, m_out, LEARN_RATE)
        q_rows = q_out.shape[0]
        q_out[...] = (sfw[i, :, pl.ds(pl.multiple_of(part * q_rows, q_rows), q_rows)] * dinv).T


def dense_update(mats, pw, sfw, dinv):
    args = [a for grp in mats for a in grp] + [pw, sfw, dinv]
    rows, cols = mats[0][0].shape
    blk = pl.BlockSpec((rows // DENSE_STEPS, cols), lambda s: (s, 0))
    q_blk = pl.BlockSpec((cols // DENSE_STEPS, 128), lambda s: (s, 0))
    in_specs = [blk] * 12 + [pl.BlockSpec((4, 128, rows // DENSE_STEPS), lambda s: (0, 0, s)),
                             pl.BlockSpec(sfw.shape, lambda s: (0, 0, 0)),
                             pl.BlockSpec(dinv.shape, lambda s: (0, 0))]
    w_out = jax.ShapeDtypeStruct((rows, cols), F32)
    return pl.pallas_call(
        dense_kernel, grid=(DENSE_STEPS,), in_specs=in_specs, out_specs=[blk, blk, q_blk] * 4,
        out_shape=[w_out, w_out, jax.ShapeDtypeStruct((cols, 128), F32)] * 4,
        compiler_params=pltpu.CompilerParams(vmem_limit_bytes=60 * MIB),
        name='dense_update',
    )(*args)


def solution(mesh):
    dense_w = P(('layer', 'fsdp'), 'tp')
    dense_f = P(('layer', 'tp'), None)
    stack_w = P('layer', 'fsdp', 'tp')
    stack_f = P('layer', 'tp', None)
    down_f = P('layer', 'fsdp', None)
    in_specs = (dense_w, dense_w, dense_w, dense_f) * 4 + (stack_w, stack_w, stack_w, stack_f) * 2 + (stack_w, stack_w, stack_w, down_f)
    out_specs = (dense_w, dense_w, dense_f) * 4 + (stack_w, stack_w, stack_f) * 2 + (stack_w, stack_w, down_f)

    def local_step(*blocks):
        dense = [blocks[4 * i:4 * i + 4] for i in range(4)]
        experts = []
        for i in (4, 5, 6):
            w, m, g, q = blocks[4 * i:4 * i + 4]
            if i < 6:
                w, m, g = (a.swapaxes(1, 2) for a in (w, m, g))
            experts.append((w, m, g, q.swapaxes(1, 2)))
        pk, pf, sf, sd, pw, sfw, dinv = exchange([grp[1:] for grp in experts], [grp[1:] for grp in dense])
        results = list(dense_update([grp[:3] for grp in dense], pw, sfw, dinv))
        out = list(expert_update([grp[:3] for grp in experts], (pk, pf, sf, sd, dinv)))
        for n in range(9):
            if n < 6 or n == 8:
                out[n] = out[n].swapaxes(1, 2)
        return tuple(results + out)

    return jax.shard_map(local_step, mesh=mesh, in_specs=in_specs, out_specs=out_specs, check_vma=False)
```

```python
import math
import jax
import jax.numpy as jnp
from jax import lax
from jax.experimental import pallas as pl
from jax.experimental.pallas import tpu as pltpu
from jax.sharding import PartitionSpec as P

MOMENTUM = 0.9
LEARN_RATE = 0.3
LANES = 128
BF = jnp.bfloat16
F32 = jnp.float32
MIB = 2 ** 20
NN = (((1,), (0,)), ((), ()))
NT = (((1,), (1,)), ((), ()))
MESH = pl.DeviceIdType.MESH


def split3(x):
    hi = x.astype(BF)
    rest = x - hi.astype(F32)
    mid = rest.astype(BF)
    low = (rest - mid.astype(F32)).astype(BF)
    return hi, mid, low


def rows_to(x, rows):
    have, cols = x.shape
    if have == rows:
        return x
    return jnp.concatenate([x, jnp.zeros((rows - have, cols), x.dtype)], axis=0)


def dot6(left, right, dims):
    rank = left.shape[0]
    pad = -(-rank // 16) * 16
    lh, lm, ll = split3(rows_to(left, pad))
    rh, rm, rl = split3(right)
    with_h = lax.dot_general(jnp.concatenate([lh, lm, ll], axis=0), rh, dims, preferred_element_type=F32)
    with_m = lax.dot_general(jnp.concatenate([lh, lm], axis=0), rm, dims, preferred_element_type=F32)
    with_l = lax.dot_general(lh, rl, dims, preferred_element_type=F32)
    small = with_h[2 * pad:2 * pad + rank] + with_m[pad:pad + rank] + with_l[:rank]
    mid = with_h[pad:pad + rank] + with_m[:rank]
    return (small + mid) + with_h[:rank]


def eliminate(a, li, rank):
    lane = lax.broadcasted_iota(jnp.int32, (8, LANES), 1)

    def pick(x, hit):
        return jnp.sum(jnp.where(hit, x, 0.0), axis=-1, keepdims=True)

    for k0 in range(0, rank, 8):
        def step(kk, carry, k0=k0):
            k = k0 + 2 * kk
            h0, h1 = lane == k, lane == k + 1
            r0, r1 = a[k], a[k + 1]
            v00, v01, v10, v11 = pick(r0, h0), pick(r0, h1), pick(r1, h0), pick(r1, h1)
            rinv0 = 1.0 / v00
            rs0 = 1.0 / jnp.sqrt(v00)
            s01 = v01 * rinv0
            sc0 = jnp.where(h0, rinv0, r0 * rinv0)
            li[k] = jnp.where(h0, rs0, jnp.where(lane < k, r0 * rs0, 0.0))
            piv1 = v11 - v10 * s01
            rinv1 = 1.0 / piv1
            rs1 = 1.0 / jnp.sqrt(piv1)
            r1 = jnp.where(h0, 0.0, r1) - v10 * sc0
            sc1 = jnp.where(h1, rinv1, r1 * rinv1)
            li[k + 1] = jnp.where(h1, rs1, jnp.where(lane < k + 1, r1 * rs1, 0.0))
            sc0 = jnp.where(h1, 0.0, sc0)

            def below(lo, n, masked):
                lane_n = lax.broadcasted_iota(jnp.int32, (n, 8, LANES), 2)
                g_hit0, g_hit1 = lane_n == k, lane_n == k + 1
                cur = a[lo:lo + n]
                g0 = pick(cur, g_hit0)
                g1 = pick(cur, g_hit1) - g0 * s01[None]
                new = jnp.where(jnp.logical_or(g_hit0, g_hit1), 0.0, cur) - g0 * sc0[None] - g1 * sc1[None]
                if masked:
                    row = lo + lax.broadcasted_iota(jnp.int32, (n, 8, LANES), 0)
                    new = jnp.where(row > k + 1, new, cur)
                a[lo:lo + n] = new

            below(k0, 8, True)
            if rank > k0 + 8:
                below(k0 + 8, rank - k0 - 8, False)
            return carry
        lax.fori_loop(0, 4, step, 0)


HELD = 5


def exchange_kernel(*refs):
    em, eg, eq = refs[0:9:3], refs[1:9:3], refs[2:9:3]
    dm, dg, dq = refs[9:21:3], refs[10:21:3], refs[11:21:3]
    o_pk, o_pf, o_sf, o_sd, o_pd, o_sfd, o_nrm = refs[21:28]
    (mk, gk, qk, md, gd, qd, mw, gw, qw,
     pk, pk_in, pd, pd_c, pd_x, pf, sk, sk_c, sk_x, sk_o, wk, wk_c, wk_x, sd, sd_in, wd, wd_in,
     pw, pw_in, sw, sw_c, sw_x, sfw, ae, li, aw, lw, nrm, nrm_y, nrm_d, nrm_f,
     ld, ldw, ldq, out_sem, outw_sem, remote, remote_w, remote_n) = refs[28:]
    t = lax.axis_index('tp')
    f = lax.axis_index('fsdp')
    c = lax.rem(f, 2)
    y_dev = {'tp': 1 - t}
    c_dev = {'fsdp': f + 1 - 2 * c}
    x_dev = {'fsdp': lax.rem(f + 2, 4)}
    xc_dev = {'fsdp': lax.rem(f + 3 - 2 * c, 4)}
    yc_dev = {'tp': 1 - t, 'fsdp': f + 1 - 2 * c}
    bar = pltpu.get_barrier_semaphore()
    for dev in (y_dev, c_dev, x_dev, xc_dev, yc_dev):
        pl.semaphore_signal(bar, inc=1, device_id=dev, device_id_type=MESH)

    def expert_load(j, e, with_q):
        m_buf, g_buf, q_buf = (mk.at[j], gk.at[j], qk.at[j]) if j < 2 else (md, gd, qd)
        slot = lax.rem(e, 2)
        m_buf, g_buf, q_buf = m_buf.at[slot], g_buf.at[slot], q_buf.at[slot]
        copies = [pltpu.make_async_copy(em[j].at[e], m_buf, ld.at[j, 0, slot]),
                  pltpu.make_async_copy(eg[j].at[e], g_buf, ld.at[j, 1, slot])]
        if with_q:
            copies.append(pltpu.make_async_copy(eq[j].at[e], q_buf, ld.at[j, 2, slot]))
        return copies

    def start_all(copies):
        for cp in copies:
            cp.start()

    def wait_all(copies):
        for cp in copies:
            cp.wait()

    def dense_load(i, s):
        slot = lax.rem(s, 2)
        rows = pl.ds(pl.multiple_of(slot * 256, 256), 256)
        return [pltpu.make_async_copy(dm[i].at[rows], mw.at[slot], ldw.at[slot, 0]),
                pltpu.make_async_copy(dg[i].at[rows], gw.at[slot], ldw.at[slot, 1])]

    def dense_q(i, s):
        slot = lax.rem(s // 2, 2)
        return pltpu.make_async_copy(dq[i], qw.at[slot], ldq.at[slot])

    def dense_start(s, with_q):
        for i in range(4):
            @pl.when(s // 2 == i)
            def _():
                start_all(dense_load(i, s))
        if with_q:
            for i in range(4):
                @pl.when(jnp.logical_and(s // 2 == i, lax.rem(s, 2) == 0))
                def _():
                    dense_q(i, s).start()

    def send(src, dst, kind, e, dev):
        return pltpu.make_async_remote_copy(src_ref=src, dst_ref=dst, send_sem=remote.at[0, kind, e],
                                            recv_sem=remote.at[1, kind, e], device_id=dev, device_id_type=MESH)

    def send_w(src, dst, kind, i, dev):
        return pltpu.make_async_remote_copy(src_ref=src, dst_ref=dst, send_sem=remote_w.at[0, kind, i],
                                            recv_sem=remote_w.at[1, kind, i], device_id=dev, device_id_type=MESH)

    def send_n(dst, kind, dev):
        return pltpu.make_async_remote_copy(src_ref=nrm, dst_ref=dst, send_sem=remote_n.at[0, kind],
                                            recv_sem=remote_n.at[1, kind], device_id=dev, device_id_type=MESH)

    def r_pk(e, j):
        return send(pk.at[e, j], pk_in.at[e, j], j, e, y_dev)

    def r_pd_c(e):
        return send(pd.at[e, 1 - c], pd_c.at[e], 2, e, c_dev)

    def r_pd_x(e):
        return send(pd.at[e, c], pd_x.at[e], 3, e, x_dev)

    def r_pd_o(e):
        return send(pf.at[e, c], pf.at[e, c], 4, e, c_dev)

    def r_sk_c(e):
        return send(sk.at[e, 1 - c], sk_c.at[e], 5, e, c_dev)

    def r_sk_x(e):
        return send(sk.at[e, c], sk_x.at[e, :, 0:768], 6, e, x_dev)

    def r_sk_o(e):
        return send(sk_x.at[e], sk_o.at[e], 7, e, c_dev)

    def r_wk_c(e):
        return send(wk.at[e, 1 - c], wk_c.at[e], 10, e, c_dev)

    def r_wk_x(e):
        return send(wk.at[e, c], wk_x.at[e], 11, e, x_dev)

    def r_sd(e):
        return send(sd.at[e], sd_in.at[e, :, 0:384], 8, e, y_dev)

    def r_wd(e):
        return send(wd.at[e], wd_in.at[e], 9, e, y_dev)

    def r_pw(i):
        return send_w(pw.at[i], pw_in.at[i], 0, i, y_dev)

    def r_sw_c(d):
        return send_w(sw.at[2 * d + 1 - c], sw_c.at[d], 1, d, c_dev)

    def r_sw_x(d):
        return send_w(sw.at[2 * d + c], sw_x.at[d], 2, d, x_dev)

    def r_sw_o(d):
        return send_w(sfw.at[2 * d + c], sfw.at[2 * d + c], 3, d, c_dev)

    def out_pk(e):
        return pltpu.make_async_copy(pk_in.at[e], o_pk.at[e], out_sem.at[0, e])

    def out_pf(e):
        return pltpu.make_async_copy(pf.at[e], o_pf.at[e], out_sem.at[1, e])

    def out_own(e):
        return pltpu.make_async_copy(sk_x.at[e], o_sf.at[e, c], out_sem.at[2, e])

    def out_other(e):
        return pltpu.make_async_copy(sk_o.at[e], o_sf.at[e, 1 - c], out_sem.at[3, e])

    def out_sd(e):
        return pltpu.make_async_copy(sd_in.at[e], o_sd.at[e], out_sem.at[4, e])

    def out_pw(i):
        return pltpu.make_async_copy(pw_in.at[i], o_pd.at[i], outw_sem.at[0, i])

    def out_sfw(i):
        return pltpu.make_async_copy(sfw.at[i], o_sfd.at[i], outw_sem.at[1, i])

    def block(j, e):
        slot = lax.rem(e, 2)
        if j < 2:
            return mk[j, slot] + gk[j, slot].astype(F32)
        return md[slot] + gd[slot].astype(F32)

    for e in range(2):
        for j in (2, 0, 1):
            start_all(expert_load(j, e, True))
    dense_start(0, True)
    pl.semaphore_wait(bar, 5)

    def dense_one(s, carry):
        slot = lax.rem(s, 2)
        i = s // 2

        @pl.when(s < 7)
        def _():
            dense_start(s + 1, True)
        wait_all(dense_load(0, s))

        @pl.when(slot == 0)
        def _():
            dense_q(0, s).wait()
        b = mw[slot] + gw[slot].astype(F32)
        cols = pl.ds(pl.multiple_of(slot * 256, 256), 256)
        pw[i, :, cols] = dot6(qw[lax.rem(i, 2)].T, b, NT)

        @pl.when(slot == 1)
        def _():
            r_pw(i).start()
        return carry


    def pd_mid(e):
        r_pd_c(e).wait_recv()
        pd[e, c] = pd[e, c] + pd_c[e]
        r_pd_x(e).start()

    def expert_one(e, carry):
        for j in (2, 0, 1):
            wait_all(expert_load(j, e, True))
            slot = lax.rem(e, 2)
            q = qk[j, slot] if j < 2 else qd[slot]
            part = dot6(q, block(j, e), NN)

            @pl.when(e < 6)
            def _(j=j):
                start_all(expert_load(j, e + 2, True))
            if j < 2:
                pk[e, j] = part

                @pl.when(e < HELD)
                def _(j=j):
                    r_pk(e, j).start()
            else:
                pd[e, 0] = part[:, :512]
                pd[e, 1] = part[:, 512:]
                r_pd_c(e).start()
        pd_mid(e)
        return carry

    lax.fori_loop(0, 2, expert_one, 0)
    lax.fori_loop(0, 8, dense_one, 0)
    lax.fori_loop(2, 8, expert_one, 0)
    for e in range(2):
        for j in range(3):
            start_all(expert_load(j, e, False))
    dense_start(0, False)

    def dense_two(s, carry):
        slot = lax.rem(s, 2)
        i = s // 2

        @pl.when(s < 7)
        def _():
            dense_start(s + 1, False)

        @pl.when(slot == 0)
        def _():
            r_pw(i).wait_recv()
            total = pw[i] + pw_in[i]
            pw_in[i] = total
            out_pw(i).start()
            sw[i, :, 1024:] = dot6(total, total, NT)
            sw[i, :, :1024] = jnp.zeros((128, 1024), F32)
        wait_all(dense_load(0, s))
        b = mw[slot] + gw[slot].astype(F32)
        cols = pl.ds(pl.multiple_of(slot * 256, 256), 256)
        sw[i, :, :1024] = sw[i, :, :1024] + dot6(pw_in[i, :, cols], b, NN)

        @pl.when(lax.rem(s, 4) == 3)
        def _():
            r_sw_c(s // 4).start()
        return carry

    def down_two(s, carry):
        @pl.when(s < 8)
        def _():
            r_pd_x(s).wait_recv()
            pf[s, c] = pd[s, c] + pd_x[s]
            r_pd_o(s).start()

        @pl.when(s > 0)
        def _():
            e = s - 1
            r_pd_o(e).wait_recv()
            out_pf(e).start()
            wait_all(expert_load(2, e, False))
            total = jnp.concatenate([pf[e, 0], pf[e, 1]], axis=1)
            wd[e] = dot6(total, rows_to(total, 128), NT)
            r_wd(e).start()
            sd[e] = dot6(total, rows_to(block(2, e), 384), NT)

            @pl.when(e < 6)
            def _():
                start_all(expert_load(2, e + 2, False))
        return carry

    def sd_send(e, carry):
        r_sd(e).start()
        return carry

    def sk_mid(e):
        r_sk_c(e).wait_recv()
        sk[e, c] = sk[e, c] + sk_c[e]
        r_sk_x(e).start()

    def keep_two(e, carry):
        for j in range(2):
            r_pk(e, j).wait_recv()
            total = pk[e, j] + pk_in[e, j]
            pk_in[e, j] = total
            wk[e, j] = dot6(total, rows_to(total, 128), NT)
        r_wk_c(e).start()
        out_pk(e).start()
        for j in range(2):
            wait_all(expert_load(j, e, False))
            sk[e, j] = dot6(pk_in[e, j], rows_to(block(j, e), 768), NT)

            @pl.when(e < 6)
            def _(j=j):
                start_all(expert_load(j, e + 2, False))
        r_sk_c(e).start()
        r_wk_c(e).wait_recv()
        wk[e, c] = wk[e, c] + wk_c[e]
        r_wk_x(e).start()

        @pl.when(e > 3)
        def _():
            sk_mid(e - 2)
        return carry

    lax.fori_loop(0, 2, keep_two, 0)
    sk_mid(0)
    sk_mid(1)
    lax.fori_loop(0, 9, down_two, 0)
    for e in range(HELD, 8):
        r_pk(e, 0).start()
        r_pk(e, 1).start()
    lax.fori_loop(0, 8, sd_send, 0)
    lax.fori_loop(0, 8, dense_two, 0)
    for d in range(2):
        r_sw_c(d).wait_recv()
        sw[2 * d + c] = sw[2 * d + c] + sw_c[d]
        r_sw_x(d).start()


    nrm[...] = jnp.zeros((128, LANES), F32)
    lane_full = lax.broadcasted_iota(jnp.int32, (128, LANES), 1)

    def add_norm(rt, where):
        sq = rows_to(jnp.sum(rt * rt, axis=1, keepdims=True), 128)
        nrm[...] = jnp.where(lane_full == where, sq, nrm[...])

    lax.fori_loop(2, 5, keep_two, 0)

    for e in range(8):
        r_wd(e).wait_recv()
        ae[:, e, :] = wd[e] + wd_in[e]
    eliminate(ae, li, 88)
    for e in range(8):
        sd_in[e, :, 384:] = li[:, e, :]

    lax.fori_loop(5, 6, keep_two, 0)

    for d in range(2):
        r_sw_x(d).wait_recv()
        sfw[2 * d + c] = sw[2 * d + c] + sw_x[d]
    for s in range(8):
        aw[:, s, :] = sfw[2 * (s % 2) + c, :, 1024:]
    eliminate(aw, lw, 128)
    for d in range(2):
        i = 2 * d + c
        inv = lw[:, d, :]
        sfw[i, :, 1024:] = inv
        rt = dot6(inv, sfw[i, :, :1024], NN)
        sfw[i, :, :1024] = rt
        add_norm(rt, 24 + i)
        r_sw_o(d).start()

    lax.fori_loop(6, 8, keep_two, 0)
    sk_mid(6)
    sk_mid(7)

    for e in range(8):
        r_wk_x(e).wait_recv()
        ae[:, e, :] = wk[e, c] + wk_x[e]
    eliminate(ae, li, 88)
    for e in range(8):
        sk_x[e, :, 768:] = li[:, e, :]

    def keep_r(e, carry):
        r_sk_x(e).wait_recv()
        st = sk[e, c] + sk_x[e, :, :768]
        rt = dot6(sk_x[e, :, 768:], rows_to(st, 128), NN)
        sk_x[e, :, :768] = rt
        r_sk_o(e).start()
        add_norm(rt, 8 * c + e)
        out_own(e).start()
        return carry

    lax.fori_loop(0, 8, keep_r, 0)

    def down_r(e, carry):
        r_sd(e).wait_recv()
        st = sd[e] + sd_in[e, :, :384]
        rt = dot6(sd_in[e, :, 384:], rows_to(st, 128), NN)
        sd_in[e, :, :384] = rt
        add_norm(rt, 16 + e)
        out_sd(e).start()
        return carry

    lax.fori_loop(0, 8, down_r, 0)

    copies = [send_n(nrm_y, 0, y_dev), send_n(nrm_d, 1, yc_dev)]
    for k in range(1, 4):
        copies.append(send_n(nrm_f.at[k - 1], k + 1, {'fsdp': lax.rem(f + k, 4)}))
    start_all(copies)

    def finish(e, carry):
        r_sk_o(e).wait_recv()
        out_other(e).start()
        return carry

    lax.fori_loop(0, 8, finish, 0)
    for d in range(2):
        out_sfw(2 * d + c).start()
        r_sw_o(d).wait_recv()
        out_sfw(2 * d + 1 - c).start()
    wait_all(copies)
    own = nrm[...]
    over_f = jnp.zeros((128, LANES), F32)
    for dev in range(4):
        k = lax.rem(f - dev + 4, 4)
        over_f = over_f + jnp.where(k == 0, own, jnp.where(k == 1, nrm_f[0], jnp.where(k == 2, nrm_f[1], nrm_f[2])))
    core = jnp.where(c == 0, nrm_f[2], nrm_f[0])
    owner = jnp.where(lane_full < 24, lane_full // 8, lax.rem(lane_full, 2))
    keep = jnp.where(owner == c, own + nrm_y[...], core + nrm_d[...])
    is_down = jnp.logical_and(lane_full >= 16, lane_full < 24)
    total = jnp.where(is_down, over_f, keep)
    nrm[...] = 1.0 / jnp.sqrt(total)
    last = pltpu.make_async_copy(nrm, o_nrm, outw_sem.at[0, 4])
    last.start()

    def drain(e, carry):
        for r in (r_pk(e, 0), r_pk(e, 1), r_pd_c(e), r_pd_x(e), r_pd_o(e), r_sk_c(e), r_sk_x(e), r_sk_o(e), r_sd(e), r_wd(e), r_wk_c(e), r_wk_x(e)):
            r.wait_send()
        for o in (out_pk(e), out_pf(e), out_own(e), out_other(e), out_sd(e)):
            o.wait()
        return carry

    lax.fori_loop(0, 8, drain, 0)
    for i in range(4):
        r_pw(i).wait_send()
        out_pw(i).wait()
        out_sfw(i).wait()
    for d in range(2):
        r_sw_c(d).wait_send()
        r_sw_x(d).wait_send()
        r_sw_o(d).wait_send()
    last.wait()


def exchange(experts, dense):
    any_spec = pl.BlockSpec(memory_space=pl.ANY)
    args = [a for grp in experts for a in grp] + [a for grp in dense for a in grp]
    shapes = [(8, 2, 88, 512), (8, 2, 88, 512), (8, 2, 88, 896), (8, 88, 512), (4, 128, 512), (4, 128, 1152), (128, 128)]
    dma = pltpu.SemaphoreType.DMA

    def v(*shape, dtype=F32):
        return pltpu.VMEM(shape, dtype)

    scratch = [v(2, 2, 704, 512), v(2, 2, 704, 512, dtype=BF), v(2, 2, 88, 704),
               v(2, 352, 1024), v(2, 352, 1024, dtype=BF), v(2, 88, 352),
               v(2, 256, 1024), v(2, 256, 1024, dtype=BF), v(2, 1024, 128),
               v(8, 2, 88, 512), v(8, 2, 88, 512),
               v(8, 2, 88, 512), v(8, 88, 512), v(8, 88, 512), v(8, 2, 88, 512),
               v(8, 2, 88, 768), v(8, 88, 768), v(8, 88, 896), v(8, 88, 896),
               v(8, 2, 88, 128), v(8, 88, 128), v(8, 88, 128),
               v(8, 88, 384), v(8, 88, 512), v(8, 88, 128), v(8, 88, 128),
               v(4, 128, 512), v(4, 128, 512), v(4, 128, 1152), v(2, 128, 1152), v(2, 128, 1152), v(4, 128, 1152),
               v(88, 8, 128), v(88, 8, 128), v(128, 8, 128), v(128, 8, 128),
               v(128, 128), v(128, 128), v(128, 128), v(3, 128, 128),
               dma((3, 3, 2)), dma((2, 2)), dma((2,)), dma((5, 8)), dma((2, 5)), dma((2, 12, 8)), dma((2, 4, 4)), dma((2, 5))]
    return pl.pallas_call(
        exchange_kernel,
        in_specs=[any_spec] * len(args), out_specs=[any_spec] * len(shapes),
        out_shape=[jax.ShapeDtypeStruct(s, F32) for s in shapes],
        scratch_shapes=scratch,
        compiler_params=pltpu.CompilerParams(collective_id=0, has_side_effects=True, vmem_limit_bytes=67043328),
        name='exchange',
    )(*args)


def left_cat(ut):
    h, m, l = split3(rows_to(ut, LANES).T)
    return jnp.concatenate([h, l, m, m, h, h], axis=1)


def right_cat(vt):
    h, m, l = split3(rows_to(vt, LANES))
    return jnp.concatenate([l, h, m, h, m, h], axis=0)


def take_col(dinv_ref, rank, where):
    lane = lax.broadcasted_iota(jnp.int32, (rank, LANES), 1)
    return jnp.sum(jnp.where(lane == where, dinv_ref[:rank, :], 0.0), axis=1, keepdims=True)


def apply_update(x_ref, m_ref, g_ref, ut, vt, dinv, x_out, m_out, scale):
    left = left_cat(ut)
    b = m_ref[...] + g_ref[...].astype(F32)
    m_out[...] = b - (1.0 - MOMENTUM) * jnp.dot(left, right_cat(vt), preferred_element_type=F32)
    x_out[...] = x_ref[...] - scale * jnp.dot(left, right_cat(vt * dinv), preferred_element_type=F32)


def expert_kernel(*refs):
    e = pl.program_id(0)
    pk, pf, sf, sd, dinv_ref = refs[9:14]
    scale = LEARN_RATE * math.sqrt(2048 / 1408)
    for j in range(3):
        x_ref, m_ref, g_ref = (r.at[0] for r in refs[3 * j:3 * j + 3])
        x_out, m_out, q_out = (r.at[0] for r in refs[14 + 3 * j:17 + 3 * j])
        dinv = take_col(dinv_ref, 88, 8 * j + e)
        if j < 2:
            pt, rt, inv = pk[0, j], sf[0, j, :, :704], sf[0, j, :, 768:]
        else:
            pt, rt, inv = jnp.concatenate([pf[0, 0], pf[0, 1]], axis=1), sd[0, :, :352], sd[0, :, 384:]
        pt = dot6(inv, rows_to(pt, LANES), NN)
        apply_update(x_ref, m_ref, g_ref, rt, pt, dinv, x_out, m_out, scale)
        q_out[...] = rt * dinv


def expert_update(mats, sums):
    def blk(a):
        n = len(a.shape)
        return pl.BlockSpec((1,) + a.shape[1:], lambda e: (e,) + (0,) * (n - 1))

    args = [a for grp in mats for a in grp] + list(sums)
    in_specs = [blk(a) for a in args[:-1]] + [pl.BlockSpec((128, 128), lambda e: (0, 0))]
    out_shape = []
    for x, _, _ in mats:
        q_shape = (8, 88, x.shape[1])
        out_shape += [jax.ShapeDtypeStruct(s, F32) for s in (x.shape, x.shape, q_shape)]
    return pl.pallas_call(
        expert_kernel, grid=(8,), in_specs=in_specs, out_specs=[blk(o) for o in out_shape], out_shape=out_shape,
        compiler_params=pltpu.CompilerParams(vmem_limit_bytes=62 * MIB),
        name='expert_update',
    )(*args)


DENSE_STEPS = 4


def dense_kernel(*refs):
    pw, linv, rt_ref, dinv_ref = refs[12:16]
    left = refs[28]

    @pl.when(pl.program_id(0) == 0)
    def _():
        for i in range(4):
            left[i] = left_cat(dot6(linv[i], pw[i], NN))

    for i in range(4):
        x_ref, m_ref, g_ref = refs[3 * i:3 * i + 3]
        x_out, m_out, q_out = refs[16 + 3 * i:19 + 3 * i]
        rt = rt_ref[i]
        qt = rt * take_col(dinv_ref, 128, 24 + i)
        b = m_ref[...] + g_ref[...].astype(F32)
        m_out[...] = b - (1.0 - MOMENTUM) * jnp.dot(left[i], right_cat(rt), preferred_element_type=F32)
        x_out[...] = x_ref[...] - LEARN_RATE * jnp.dot(left[i], right_cat(qt), preferred_element_type=F32)
        q_out[...] = qt.T


def dense_update(mats, pw, sfw, dinv):
    args = [a for grp in mats for a in grp] + [pw, sfw, sfw, dinv]
    rows, cols = mats[0][0].shape
    wide = cols // DENSE_STEPS
    blk = pl.BlockSpec((rows, wide), lambda s: (0, s))
    q_blk = pl.BlockSpec((wide, 128), lambda s: (s, 0))
    in_specs = [blk] * 12 + [pl.BlockSpec(pw.shape, lambda s: (0, 0, 0)),
                             pl.BlockSpec((4, 128, 128), lambda s: (0, 0, 8)),
                             pl.BlockSpec((4, 128, wide), lambda s: (0, 0, s)),
                             pl.BlockSpec(dinv.shape, lambda s: (0, 0))]
    w_out = jax.ShapeDtypeStruct((rows, cols), F32)
    return pl.pallas_call(
        dense_kernel, grid=(DENSE_STEPS,), in_specs=in_specs, out_specs=[blk, blk, q_blk] * 4,
        out_shape=[w_out, w_out, jax.ShapeDtypeStruct((cols, 128), F32)] * 4,
        scratch_shapes=[pltpu.VMEM((4, rows, 6 * LANES), BF)],
        compiler_params=pltpu.CompilerParams(vmem_limit_bytes=60 * MIB),
        name='dense_update',
    )(*args)


def solution(mesh):
    dense_w = P(('layer', 'fsdp'), 'tp')
    dense_f = P(('layer', 'tp'), None)
    stack_w = P('layer', 'fsdp', 'tp')
    stack_f = P('layer', 'tp', None)
    down_f = P('layer', 'fsdp', None)
    in_specs = (dense_w, dense_w, dense_w, dense_f) * 4 + (stack_w, stack_w, stack_w, stack_f) * 2 + (stack_w, stack_w, stack_w, down_f)
    out_specs = (dense_w, dense_w, dense_f) * 4 + (stack_w, stack_w, stack_f) * 2 + (stack_w, stack_w, down_f)

    def local_step(*blocks):
        dense = [blocks[4 * i:4 * i + 4] for i in range(4)]
        experts = []
        for i in (4, 5, 6):
            w, m, g, q = blocks[4 * i:4 * i + 4]
            if i < 6:
                w, m, g = (a.swapaxes(1, 2) for a in (w, m, g))
            experts.append((w, m, g, q.swapaxes(1, 2)))
        pk, pf, sf, sd, pw, sfw, dinv = exchange([grp[1:] for grp in experts], [grp[1:] for grp in dense])
        results = list(dense_update([grp[:3] for grp in dense], pw, sfw, dinv))
        out = list(expert_update([grp[:3] for grp in experts], (pk, pf, sf, sd, dinv)))
        for n in range(9):
            if n < 6 or n == 8:
                out[n] = out[n].swapaxes(1, 2)
        return tuple(results + out)

    return jax.shard_map(local_step, mesh=mesh, in_specs=in_specs, out_specs=out_specs, check_vma=False)
```

```python
import math
import jax
import jax.numpy as jnp
from jax import lax
from jax.experimental import pallas as pl
from jax.experimental.pallas import tpu as pltpu
from jax.sharding import PartitionSpec as P

MOMENTUM = 0.9
LEARN_RATE = 0.3
LANES = 128
BF = jnp.bfloat16
F32 = jnp.float32
MIB = 2 ** 20
NN = (((1,), (0,)), ((), ()))
NT = (((1,), (1,)), ((), ()))
MESH = pl.DeviceIdType.MESH


def split3(x):
    hi = x.astype(BF)
    rest = x - hi.astype(F32)
    mid = rest.astype(BF)
    low = (rest - mid.astype(F32)).astype(BF)
    return hi, mid, low


def rows_to(x, rows):
    have, cols = x.shape
    if have == rows:
        return x
    return jnp.concatenate([x, jnp.zeros((rows - have, cols), x.dtype)], axis=0)


def dot6(left, right, dims, grow=0):
    rank = left.shape[0]
    pad = -(-rank // 16) * 16
    lh, lm, ll = split3(rows_to(left, pad))
    rh, rm, rl = (rows_to(term, grow) if grow else term for term in split3(right))
    with_h = lax.dot_general(jnp.concatenate([lh, lm, ll], axis=0), rh, dims, preferred_element_type=F32)
    with_m = lax.dot_general(jnp.concatenate([lh, lm], axis=0), rm, dims, preferred_element_type=F32)
    with_l = lax.dot_general(lh, rl, dims, preferred_element_type=F32)
    small = with_h[2 * pad:2 * pad + rank] + with_m[pad:pad + rank] + with_l[:rank]
    mid = with_h[pad:pad + rank] + with_m[:rank]
    return (small + mid) + with_h[:rank]


def eliminate(a, li, rank):
    lane = lax.broadcasted_iota(jnp.int32, (8, LANES), 1)

    def pick(x, hit):
        return jnp.sum(jnp.where(hit, x, 0.0), axis=-1, keepdims=True)

    for k0 in range(0, rank, 8):
        def step(kk, carry, k0=k0):
            k = k0 + 2 * kk
            h0, h1 = lane == k, lane == k + 1
            r0, r1 = a[k], a[k + 1]
            v00, v01, v10, v11 = pick(r0, h0), pick(r0, h1), pick(r1, h0), pick(r1, h1)
            rinv0 = 1.0 / v00
            rs0 = 1.0 / jnp.sqrt(v00)
            s01 = v01 * rinv0
            sc0 = jnp.where(h0, rinv0, r0 * rinv0)
            li[k] = jnp.where(h0, rs0, jnp.where(lane < k, r0 * rs0, 0.0))
            piv1 = v11 - v10 * s01
            rinv1 = 1.0 / piv1
            rs1 = 1.0 / jnp.sqrt(piv1)
            r1 = jnp.where(h0, 0.0, r1) - v10 * sc0
            sc1 = jnp.where(h1, rinv1, r1 * rinv1)
            li[k + 1] = jnp.where(h1, rs1, jnp.where(lane < k + 1, r1 * rs1, 0.0))
            sc0 = jnp.where(h1, 0.0, sc0)

            def below(lo, n, masked):
                lane_n = lax.broadcasted_iota(jnp.int32, (n, 8, LANES), 2)
                g_hit0, g_hit1 = lane_n == k, lane_n == k + 1
                cur = a[lo:lo + n]
                g0 = pick(cur, g_hit0)
                g1 = pick(cur, g_hit1) - g0 * s01[None]
                new = jnp.where(jnp.logical_or(g_hit0, g_hit1), 0.0, cur) - g0 * sc0[None] - g1 * sc1[None]
                if masked:
                    row = lo + lax.broadcasted_iota(jnp.int32, (n, 8, LANES), 0)
                    new = jnp.where(row > k + 1, new, cur)
                a[lo:lo + n] = new

            below(k0, 8, True)
            if rank > k0 + 8:
                below(k0 + 8, rank - k0 - 8, False)
            return carry
        lax.fori_loop(0, 4, step, 0)


HELD = 5


def exchange_kernel(*refs):
    em, eg, eq = refs[0:9:3], refs[1:9:3], refs[2:9:3]
    dm, dg, dq = refs[9:21:3], refs[10:21:3], refs[11:21:3]
    o_pk, o_pf, o_sf, o_sd, o_pd, o_sfd, o_nrm = refs[21:28]
    (mk, gk, qk, md, gd, qd, mw, gw, qw,
     pk, pk_in, pd, pd_c, pd_x, pf, sk, sk_c, sk_x, sk_o, wk, wk_c, wk_x, sd, sd_in, wd, wd_in,
     pw, pw_in, sw, sw_c, sw_x, sfw, ae, li, aw, lw, nrm, nrm_y, nrm_d, nrm_f,
     ld, ldw, ldq, out_sem, outw_sem, remote, remote_w, remote_n) = refs[28:]
    t = lax.axis_index('tp')
    f = lax.axis_index('fsdp')
    c = lax.rem(f, 2)
    y_dev = {'tp': 1 - t}
    c_dev = {'fsdp': f + 1 - 2 * c}
    x_dev = {'fsdp': lax.rem(f + 2, 4)}
    xc_dev = {'fsdp': lax.rem(f + 3 - 2 * c, 4)}
    yc_dev = {'tp': 1 - t, 'fsdp': f + 1 - 2 * c}
    bar = pltpu.get_barrier_semaphore()
    for dev in (y_dev, c_dev, x_dev, xc_dev, yc_dev):
        pl.semaphore_signal(bar, inc=1, device_id=dev, device_id_type=MESH)

    def expert_load(j, e, with_q):
        m_buf, g_buf, q_buf = (mk.at[j], gk.at[j], qk.at[j]) if j < 2 else (md, gd, qd)
        slot = lax.rem(e, 2)
        m_buf, g_buf, q_buf = m_buf.at[slot], g_buf.at[slot], q_buf.at[slot]
        copies = [pltpu.make_async_copy(em[j].at[e], m_buf, ld.at[j, 0, slot]),
                  pltpu.make_async_copy(eg[j].at[e], g_buf, ld.at[j, 1, slot])]
        if with_q:
            copies.append(pltpu.make_async_copy(eq[j].at[e], q_buf, ld.at[j, 2, slot]))
        return copies

    def start_all(copies):
        for cp in copies:
            cp.start()

    def wait_all(copies):
        for cp in copies:
            cp.wait()

    def dense_load(i, s):
        slot = lax.rem(s, 2)
        rows = pl.ds(pl.multiple_of(slot * 256, 256), 256)
        return [pltpu.make_async_copy(dm[i].at[rows], mw.at[slot], ldw.at[slot, 0]),
                pltpu.make_async_copy(dg[i].at[rows], gw.at[slot], ldw.at[slot, 1])]

    def dense_q(i, s):
        slot = lax.rem(s // 2, 2)
        return pltpu.make_async_copy(dq[i], qw.at[slot], ldq.at[slot])

    def dense_start(s, with_q):
        for i in range(4):
            @pl.when(s // 2 == i)
            def _():
                start_all(dense_load(i, s))
        if with_q:
            for i in range(4):
                @pl.when(jnp.logical_and(s // 2 == i, lax.rem(s, 2) == 0))
                def _():
                    dense_q(i, s).start()

    def send(src, dst, kind, e, dev):
        return pltpu.make_async_remote_copy(src_ref=src, dst_ref=dst, send_sem=remote.at[0, kind, e],
                                            recv_sem=remote.at[1, kind, e], device_id=dev, device_id_type=MESH)

    def send_w(src, dst, kind, i, dev):
        return pltpu.make_async_remote_copy(src_ref=src, dst_ref=dst, send_sem=remote_w.at[0, kind, i],
                                            recv_sem=remote_w.at[1, kind, i], device_id=dev, device_id_type=MESH)

    def send_n(dst, kind, dev):
        return pltpu.make_async_remote_copy(src_ref=nrm, dst_ref=dst, send_sem=remote_n.at[0, kind],
                                            recv_sem=remote_n.at[1, kind], device_id=dev, device_id_type=MESH)

    def r_pk(e, j):
        return send(pk.at[e, j], pk_in.at[e, j], j, e, y_dev)

    def r_pd_c(e):
        return send(pd.at[e, 1 - c], pd_c.at[e], 2, e, c_dev)

    def r_pd_x(e):
        return send(pd.at[e, c], pd_x.at[e], 3, e, x_dev)

    def r_pd_o(e):
        return send(pf.at[e, c], pf.at[e, c], 4, e, c_dev)

    def r_sk_c(e):
        return send(sk.at[e, 1 - c], sk_c.at[e], 5, e, c_dev)

    def r_sk_x(e):
        return send(sk.at[e, c], sk_x.at[e, :, 0:768], 6, e, x_dev)

    def r_sk_o(e):
        return send(sk_x.at[e], sk_o.at[e], 7, e, c_dev)

    def r_wk_c(e):
        return send(wk.at[e, 1 - c], wk_c.at[e], 10, e, c_dev)

    def r_wk_x(e):
        return send(wk.at[e, c], wk_x.at[e], 11, e, x_dev)

    def r_sd(e):
        return send(sd.at[e], sd_in.at[e, :, 0:384], 8, e, y_dev)

    def r_wd(e):
        return send(wd.at[e], wd_in.at[e], 9, e, y_dev)

    def r_pw(i):
        return send_w(pw.at[i], pw_in.at[i], 0, i, y_dev)

    def r_sw_c(d):
        return send_w(sw.at[2 * d + 1 - c], sw_c.at[d], 1, d, c_dev)

    def r_sw_x(d):
        return send_w(sw.at[2 * d + c], sw_x.at[d], 2, d, x_dev)

    def r_sw_o(d):
        return send_w(sfw.at[2 * d + c], sfw.at[2 * d + c], 3, d, c_dev)

    def out_pk(e):
        return pltpu.make_async_copy(pk_in.at[e], o_pk.at[e], out_sem.at[0, e])

    def out_pf(e):
        return pltpu.make_async_copy(pf.at[e], o_pf.at[e], out_sem.at[1, e])

    def out_own(e):
        return pltpu.make_async_copy(sk_x.at[e], o_sf.at[e, c], out_sem.at[2, e])

    def out_other(e):
        return pltpu.make_async_copy(sk_o.at[e], o_sf.at[e, 1 - c], out_sem.at[3, e])

    def out_sd(e):
        return pltpu.make_async_copy(sd_in.at[e], o_sd.at[e], out_sem.at[4, e])

    def out_pw(i):
        return pltpu.make_async_copy(pw_in.at[i], o_pd.at[i], outw_sem.at[0, i])

    def out_sfw(i):
        return pltpu.make_async_copy(sfw.at[i], o_sfd.at[i], outw_sem.at[1, i])

    def block(j, e):
        slot = lax.rem(e, 2)
        if j < 2:
            return mk[j, slot] + gk[j, slot].astype(F32)
        return md[slot] + gd[slot].astype(F32)

    for e in range(2):
        for j in (2, 0, 1):
            start_all(expert_load(j, e, True))
    dense_start(0, True)
    pl.semaphore_wait(bar, 5)

    def dense_one(s, carry):
        slot = lax.rem(s, 2)
        i = s // 2

        @pl.when(s < 7)
        def _():
            dense_start(s + 1, True)
        wait_all(dense_load(0, s))

        @pl.when(slot == 0)
        def _():
            dense_q(0, s).wait()
        b = mw[slot] + gw[slot].astype(F32)
        cols = pl.ds(pl.multiple_of(slot * 256, 256), 256)
        pw[i, :, cols] = dot6(qw[lax.rem(i, 2)].T, b, NT)

        @pl.when(slot == 1)
        def _():
            r_pw(i).start()
        return carry


    def pd_mid(e):
        r_pd_c(e).wait_recv()
        pd[e, c] = pd[e, c] + pd_c[e]
        r_pd_x(e).start()

    def expert_one(e, carry):
        for j in (2, 0, 1):
            wait_all(expert_load(j, e, True))
            slot = lax.rem(e, 2)
            q = qk[j, slot] if j < 2 else qd[slot]
            part = dot6(q, block(j, e), NN)

            @pl.when(e < 6)
            def _(j=j):
                start_all(expert_load(j, e + 2, True))
            if j < 2:
                pk[e, j] = part

                @pl.when(e < HELD)
                def _(j=j):
                    r_pk(e, j).start()
            else:
                pd[e, 0] = part[:, :512]
                pd[e, 1] = part[:, 512:]
                r_pd_c(e).start()
        pd_mid(e)
        return carry

    lax.fori_loop(0, 2, expert_one, 0)
    lax.fori_loop(0, 8, dense_one, 0)
    lax.fori_loop(2, 8, expert_one, 0)
    for e in range(2):
        for j in range(3):
            start_all(expert_load(j, e, False))
    dense_start(0, False)

    def dense_two(s, carry):
        slot = lax.rem(s, 2)
        i = s // 2

        @pl.when(s < 7)
        def _():
            dense_start(s + 1, False)

        @pl.when(slot == 0)
        def _():
            r_pw(i).wait_recv()
            total = pw[i] + pw_in[i]
            pw_in[i] = total
            out_pw(i).start()
            sw[i, :, 1024:] = dot6(total, total, NT)
            sw[i, :, :1024] = jnp.zeros((128, 1024), F32)
        wait_all(dense_load(0, s))
        b = mw[slot] + gw[slot].astype(F32)
        cols = pl.ds(pl.multiple_of(slot * 256, 256), 256)
        sw[i, :, :1024] = sw[i, :, :1024] + dot6(pw_in[i, :, cols], b, NN)

        @pl.when(lax.rem(s, 4) == 3)
        def _():
            r_sw_c(s // 4).start()
        return carry

    def down_two(s, carry):
        @pl.when(s < 8)
        def _():
            r_pd_x(s).wait_recv()
            pf[s, c] = pd[s, c] + pd_x[s]
            r_pd_o(s).start()

        @pl.when(s > 0)
        def _():
            e = s - 1
            r_pd_o(e).wait_recv()
            out_pf(e).start()
            wait_all(expert_load(2, e, False))
            total = jnp.concatenate([pf[e, 0], pf[e, 1]], axis=1)
            wd[e] = dot6(total, rows_to(total, 128), NT)
            r_wd(e).start()
            sd[e] = dot6(total, block(2, e), NT, 384)

            @pl.when(e < 6)
            def _():
                start_all(expert_load(2, e + 2, False))
        return carry

    def sd_send(e, carry):
        r_sd(e).start()
        return carry

    def sk_mid(e):
        r_sk_c(e).wait_recv()
        sk[e, c] = sk[e, c] + sk_c[e]
        r_sk_x(e).start()

    def keep_two(e, carry):
        for j in range(2):
            r_pk(e, j).wait_recv()
            total = pk[e, j] + pk_in[e, j]
            pk_in[e, j] = total
            wk[e, j] = dot6(total, rows_to(total, 128), NT)
        r_wk_c(e).start()
        out_pk(e).start()
        for j in range(2):
            wait_all(expert_load(j, e, False))
            sk[e, j] = dot6(pk_in[e, j], block(j, e), NT, 768)

            @pl.when(e < 6)
            def _(j=j):
                start_all(expert_load(j, e + 2, False))
        r_sk_c(e).start()
        r_wk_c(e).wait_recv()
        wk[e, c] = wk[e, c] + wk_c[e]
        r_wk_x(e).start()

        @pl.when(e > 3)
        def _():
            sk_mid(e - 2)
        return carry

    lax.fori_loop(0, 2, keep_two, 0)
    sk_mid(0)
    sk_mid(1)
    lax.fori_loop(0, 9, down_two, 0)
    for e in range(HELD, 8):
        r_pk(e, 0).start()
        r_pk(e, 1).start()
    lax.fori_loop(0, 8, sd_send, 0)
    lax.fori_loop(0, 8, dense_two, 0)
    for d in range(2):
        r_sw_c(d).wait_recv()
        sw[2 * d + c] = sw[2 * d + c] + sw_c[d]
        r_sw_x(d).start()


    nrm[...] = jnp.zeros((128, LANES), F32)
    lane_full = lax.broadcasted_iota(jnp.int32, (128, LANES), 1)

    def add_norm(rt, where):
        sq = rows_to(jnp.sum(rt * rt, axis=1, keepdims=True), 128)
        nrm[...] = jnp.where(lane_full == where, sq, nrm[...])

    lax.fori_loop(2, 5, keep_two, 0)

    for e in range(8):
        r_wd(e).wait_recv()
        ae[:, e, :] = wd[e] + wd_in[e]
    eliminate(ae, li, 88)
    for e in range(8):
        sd_in[e, :, 384:] = li[:, e, :]

    lax.fori_loop(5, 6, keep_two, 0)

    for d in range(2):
        r_sw_x(d).wait_recv()
        sfw[2 * d + c] = sw[2 * d + c] + sw_x[d]
    for s in range(8):
        aw[:, s, :] = sfw[2 * (s % 2) + c, :, 1024:]
    eliminate(aw, lw, 128)
    for d in range(2):
        i = 2 * d + c
        inv = lw[:, d, :]
        sfw[i, :, 1024:] = inv
        rt = dot6(inv, sfw[i, :, :1024], NN)
        sfw[i, :, :1024] = rt
        add_norm(rt, 24 + i)
        r_sw_o(d).start()

    lax.fori_loop(6, 8, keep_two, 0)
    sk_mid(6)
    sk_mid(7)

    for e in range(8):
        r_wk_x(e).wait_recv()
        ae[:, e, :] = wk[e, c] + wk_x[e]
    eliminate(ae, li, 88)
    for e in range(8):
        sk_x[e, :, 768:] = li[:, e, :]

    def keep_r(e, carry):
        r_sk_x(e).wait_recv()
        st = sk[e, c] + sk_x[e, :, :768]
        rt = dot6(sk_x[e, :, 768:], rows_to(st, 128), NN)
        sk_x[e, :, :768] = rt
        r_sk_o(e).start()
        add_norm(rt, 8 * c + e)
        out_own(e).start()
        return carry

    lax.fori_loop(0, 8, keep_r, 0)

    def down_r(e, carry):
        r_sd(e).wait_recv()
        st = sd[e] + sd_in[e, :, :384]
        rt = dot6(sd_in[e, :, 384:], rows_to(st, 128), NN)
        sd_in[e, :, :384] = rt
        add_norm(rt, 16 + e)
        out_sd(e).start()
        return carry

    lax.fori_loop(0, 8, down_r, 0)

    copies = [send_n(nrm_y, 0, y_dev), send_n(nrm_d, 1, yc_dev)]
    for k in range(1, 4):
        copies.append(send_n(nrm_f.at[k - 1], k + 1, {'fsdp': lax.rem(f + k, 4)}))
    start_all(copies)

    def finish(e, carry):
        r_sk_o(e).wait_recv()
        out_other(e).start()
        return carry

    lax.fori_loop(0, 8, finish, 0)
    for d in range(2):
        out_sfw(2 * d + c).start()
        r_sw_o(d).wait_recv()
        out_sfw(2 * d + 1 - c).start()
    wait_all(copies)
    own = nrm[...]
    over_f = jnp.zeros((128, LANES), F32)
    for dev in range(4):
        k = lax.rem(f - dev + 4, 4)
        over_f = over_f + jnp.where(k == 0, own, jnp.where(k == 1, nrm_f[0], jnp.where(k == 2, nrm_f[1], nrm_f[2])))
    core = jnp.where(c == 0, nrm_f[2], nrm_f[0])
    owner = jnp.where(lane_full < 24, lane_full // 8, lax.rem(lane_full, 2))
    keep = jnp.where(owner == c, own + nrm_y[...], core + nrm_d[...])
    is_down = jnp.logical_and(lane_full >= 16, lane_full < 24)
    total = jnp.where(is_down, over_f, keep)
    nrm[...] = 1.0 / jnp.sqrt(total)
    last = pltpu.make_async_copy(nrm, o_nrm, outw_sem.at[0, 4])
    last.start()

    def drain(e, carry):
        for r in (r_pk(e, 0), r_pk(e, 1), r_pd_c(e), r_pd_x(e), r_pd_o(e), r_sk_c(e), r_sk_x(e), r_sk_o(e), r_sd(e), r_wd(e), r_wk_c(e), r_wk_x(e)):
            r.wait_send()
        for o in (out_pk(e), out_pf(e), out_own(e), out_other(e), out_sd(e)):
            o.wait()
        return carry

    lax.fori_loop(0, 8, drain, 0)
    for i in range(4):
        r_pw(i).wait_send()
        out_pw(i).wait()
        out_sfw(i).wait()
    for d in range(2):
        r_sw_c(d).wait_send()
        r_sw_x(d).wait_send()
        r_sw_o(d).wait_send()
    last.wait()


def exchange(experts, dense):
    any_spec = pl.BlockSpec(memory_space=pl.ANY)
    args = [a for grp in experts for a in grp] + [a for grp in dense for a in grp]
    shapes = [(8, 2, 88, 512), (8, 2, 88, 512), (8, 2, 88, 896), (8, 88, 512), (4, 128, 512), (4, 128, 1152), (128, 128)]
    dma = pltpu.SemaphoreType.DMA

    def v(*shape, dtype=F32):
        return pltpu.VMEM(shape, dtype)

    scratch = [v(2, 2, 704, 512), v(2, 2, 704, 512, dtype=BF), v(2, 2, 88, 704),
               v(2, 352, 1024), v(2, 352, 1024, dtype=BF), v(2, 88, 352),
               v(2, 256, 1024), v(2, 256, 1024, dtype=BF), v(2, 1024, 128),
               v(8, 2, 88, 512), v(8, 2, 88, 512),
               v(8, 2, 88, 512), v(8, 88, 512), v(8, 88, 512), v(8, 2, 88, 512),
               v(8, 2, 88, 768), v(8, 88, 768), v(8, 88, 896), v(8, 88, 896),
               v(8, 2, 88, 128), v(8, 88, 128), v(8, 88, 128),
               v(8, 88, 384), v(8, 88, 512), v(8, 88, 128), v(8, 88, 128),
               v(4, 128, 512), v(4, 128, 512), v(4, 128, 1152), v(2, 128, 1152), v(2, 128, 1152), v(4, 128, 1152),
               v(88, 8, 128), v(88, 8, 128), v(128, 8, 128), v(128, 8, 128),
               v(128, 128), v(128, 128), v(128, 128), v(3, 128, 128),
               dma((3, 3, 2)), dma((2, 2)), dma((2,)), dma((5, 8)), dma((2, 5)), dma((2, 12, 8)), dma((2, 4, 4)), dma((2, 5))]
    return pl.pallas_call(
        exchange_kernel,
        in_specs=[any_spec] * len(args), out_specs=[any_spec] * len(shapes),
        out_shape=[jax.ShapeDtypeStruct(s, F32) for s in shapes],
        scratch_shapes=scratch,
        compiler_params=pltpu.CompilerParams(collective_id=0, has_side_effects=True, vmem_limit_bytes=67043328),
        name='exchange',
    )(*args)


def left_cat(ut):
    h, m, l = split3(rows_to(ut, LANES).T)
    return jnp.concatenate([h, l, m, m, h, h], axis=1)


def right_cat(vt):
    h, m, l = split3(rows_to(vt, LANES))
    return jnp.concatenate([l, h, m, h, m, h], axis=0)


def take_col(dinv_ref, rank, where):
    lane = lax.broadcasted_iota(jnp.int32, (rank, LANES), 1)
    return jnp.sum(jnp.where(lane == where, dinv_ref[:rank, :], 0.0), axis=1, keepdims=True)


def apply_update(x_ref, m_ref, g_ref, ut, vt, dinv, x_out, m_out, scale):
    left = left_cat(ut)
    b = m_ref[...] + g_ref[...].astype(F32)
    m_out[...] = b - (1.0 - MOMENTUM) * jnp.dot(left, right_cat(vt), preferred_element_type=F32)
    x_out[...] = x_ref[...] - scale * jnp.dot(left, right_cat(vt * dinv), preferred_element_type=F32)


def expert_kernel(*refs):
    e = pl.program_id(0)
    pk, pf, sf, sd, dinv_ref = refs[9:14]
    scale = LEARN_RATE * math.sqrt(2048 / 1408)
    for j in range(3):
        x_ref, m_ref, g_ref = (r.at[0] for r in refs[3 * j:3 * j + 3])
        x_out, m_out, q_out = (r.at[0] for r in refs[14 + 3 * j:17 + 3 * j])
        dinv = take_col(dinv_ref, 88, 8 * j + e)
        if j < 2:
            pt, rt, inv = pk[0, j], sf[0, j, :, :704], sf[0, j, :, 768:]
        else:
            pt, rt, inv = jnp.concatenate([pf[0, 0], pf[0, 1]], axis=1), sd[0, :, :352], sd[0, :, 384:]
        pt = dot6(inv, rows_to(pt, LANES), NN)
        apply_update(x_ref, m_ref, g_ref, rt, pt, dinv, x_out, m_out, scale)
        q_out[...] = rt * dinv


def expert_update(mats, sums):
    def blk(a):
        n = len(a.shape)
        return pl.BlockSpec((1,) + a.shape[1:], lambda e: (e,) + (0,) * (n - 1))

    args = [a for grp in mats for a in grp] + list(sums)
    in_specs = [blk(a) for a in args[:-1]] + [pl.BlockSpec((128, 128), lambda e: (0, 0))]
    out_shape = []
    for x, _, _ in mats:
        q_shape = (8, 88, x.shape[1])
        out_shape += [jax.ShapeDtypeStruct(s, F32) for s in (x.shape, x.shape, q_shape)]
    return pl.pallas_call(
        expert_kernel, grid=(8,), in_specs=in_specs, out_specs=[blk(o) for o in out_shape], out_shape=out_shape,
        compiler_params=pltpu.CompilerParams(vmem_limit_bytes=62 * MIB),
        name='expert_update',
    )(*args)


DENSE_STEPS = 4


def dense_kernel(*refs):
    pw, linv, rt_ref, dinv_ref = refs[12:16]
    left = refs[28]

    @pl.when(pl.program_id(0) == 0)
    def _():
        for i in range(4):
            left[i] = left_cat(dot6(linv[i], pw[i], NN))

    for i in range(4):
        x_ref, m_ref, g_ref = refs[3 * i:3 * i + 3]
        x_out, m_out, q_out = refs[16 + 3 * i:19 + 3 * i]
        rt = rt_ref[i]
        qt = rt * take_col(dinv_ref, 128, 24 + i)
        b = m_ref[...] + g_ref[...].astype(F32)
        m_out[...] = b - (1.0 - MOMENTUM) * jnp.dot(left[i], right_cat(rt), preferred_element_type=F32)
        x_out[...] = x_ref[...] - LEARN_RATE * jnp.dot(left[i], right_cat(qt), preferred_element_type=F32)
        q_out[...] = qt.T


def dense_update(mats, pw, sfw, dinv):
    args = [a for grp in mats for a in grp] + [pw, sfw, sfw, dinv]
    rows, cols = mats[0][0].shape
    wide = cols // DENSE_STEPS
    blk = pl.BlockSpec((rows, wide), lambda s: (0, s))
    q_blk = pl.BlockSpec((wide, 128), lambda s: (s, 0))
    in_specs = [blk] * 12 + [pl.BlockSpec(pw.shape, lambda s: (0, 0, 0)),
                             pl.BlockSpec((4, 128, 128), lambda s: (0, 0, 8)),
                             pl.BlockSpec((4, 128, wide), lambda s: (0, 0, s)),
                             pl.BlockSpec(dinv.shape, lambda s: (0, 0))]
    w_out = jax.ShapeDtypeStruct((rows, cols), F32)
    return pl.pallas_call(
        dense_kernel, grid=(DENSE_STEPS,), in_specs=in_specs, out_specs=[blk, blk, q_blk] * 4,
        out_shape=[w_out, w_out, jax.ShapeDtypeStruct((cols, 128), F32)] * 4,
        scratch_shapes=[pltpu.VMEM((4, rows, 6 * LANES), BF)],
        compiler_params=pltpu.CompilerParams(vmem_limit_bytes=60 * MIB),
        name='dense_update',
    )(*args)


def solution(mesh):
    dense_w = P(('layer', 'fsdp'), 'tp')
    dense_f = P(('layer', 'tp'), None)
    stack_w = P('layer', 'fsdp', 'tp')
    stack_f = P('layer', 'tp', None)
    down_f = P('layer', 'fsdp', None)
    in_specs = (dense_w, dense_w, dense_w, dense_f) * 4 + (stack_w, stack_w, stack_w, stack_f) * 2 + (stack_w, stack_w, stack_w, down_f)
    out_specs = (dense_w, dense_w, dense_f) * 4 + (stack_w, stack_w, stack_f) * 2 + (stack_w, stack_w, down_f)

    def local_step(*blocks):
        dense = [blocks[4 * i:4 * i + 4] for i in range(4)]
        experts = []
        for i in (4, 5, 6):
            w, m, g, q = blocks[4 * i:4 * i + 4]
            if i < 6:
                w, m, g = (a.swapaxes(1, 2) for a in (w, m, g))
            experts.append((w, m, g, q.swapaxes(1, 2)))
        pk, pf, sf, sd, pw, sfw, dinv = exchange([grp[1:] for grp in experts], [grp[1:] for grp in dense])
        results = list(dense_update([grp[:3] for grp in dense], pw, sfw, dinv))
        out = list(expert_update([grp[:3] for grp in experts], (pk, pf, sf, sd, dinv)))
        for n in range(9):
            if n < 6 or n == 8:
                out[n] = out[n].swapaxes(1, 2)
        return tuple(results + out)

    return jax.shard_map(local_step, mesh=mesh, in_specs=in_specs, out_specs=out_specs, check_vma=False)
```
